256 devices in a mesh: gx: 4 (over x), gy: 4 (over y), gz: 16 (over z, core).
Axes of the slice: x: 4, y: 4, z: 8, core: 2. Of those that a mesh axis runs over, the one named last changes fastest.
Arguments:
- snapshots: bfloat16 [64, 3, 32, 128, 512], P(None, None, 'gy', 'gz', 'gx'), may hold values from -6 to 6
- modes: bfloat16 [128, 3, 32, 128, 512], P(None, None, 'gy', 'gz', 'gx'), may hold values from -0.0024414062 to 0.0024414062
Outputs:
- reduced_snapshots: float32 [128, 64], replicated
- reduced_features: float32 [128, 64], replicated
- gram_snap: float32 [128, 128], replicated
- gram_feature: float32 [128, 128], replicated
- gram_quad: float32 [64, 64], replicated
The draws below stay inside these ranges and needn't reach their ends.
All inputs are finite; a program needn't handle non-finite values.
Results may differ from the reference program's by a relative error of at most 0.0029.
Values may be sent and summed in bfloat16 or wider, within the bound.
No kernel may reach another device: no remote copies, remote signals or barrier semaphores. Data moves between devices by JAX's collectives and lax.ppermute only.
A program may use at most 128 MiB of HBM per device.

```python
import jax
import jax.numpy as jnp
from jax import lax

MODES = 128
SNAPS = 64
NX = 512
NY = 32
NZ = 128


def levels(rng, shape, cuts, smallest, largest):
    def one(position, shards_of):
        heights = jax.random.uniform(jax.random.fold_in(jax.random.fold_in(rng, 6), position), (shards_of,), jnp.float32, smallest / len(cuts), largest / len(cuts))
        return jnp.repeat(jnp.exp(heights), shape[position] // shards_of).reshape((-1,) + (1,) * (len(shape) - position - 1))

    factor_of = one(*cuts[0])
    for cut in cuts[1:]:
        factor_of = factor_of * one(*cut)
    return factor_of


def bell_draw(stream_key, dims, scale, limit, shards=(), kind=jnp.bfloat16):
    array = scale * jax.random.normal(stream_key, dims, jnp.float32)
    if shards:
        array = array * levels(stream_key, dims, shards, -0.22, 0.18)
    return jnp.clip(array, -limit, limit).astype(kind)


def setup_inputs(seed: int = 0) -> dict:
    seeds = jax.random.split(jax.random.key(seed), 3)
    snapshots = bell_draw(seeds[0], (SNAPS, 3, NY, NZ, NX), 1.0, 6.0, ((2, 4), (3, 16), (4, 4)))
    modes = bell_draw(seeds[1], (MODES, 3, NY, NZ, NX), (3 * NX * NY * NZ) ** -0.5, 0.0024414062, ((2, 4), (3, 16), (4, 4)))
    return dict(snapshots=snapshots, modes=modes)


viscosity = 0.1


def stencil_terms(padded, direction, extent):
    pieces = [lax.slice_in_dim(padded, offset, offset + extent, axis=direction).astype(jnp.float32) for offset in range(5)]
    gradient = (8.0 * (pieces[3] - pieces[1]) - (pieces[4] - pieces[0])) / 12.0
    curvature = (16.0 * (pieces[3] + pieces[1]) - (pieces[4] + pieces[0]) - 30.0 * pieces[2]) / 12.0
    return gradient, curvature


def feature_field(velocity, padded_list):
    advect = jnp.zeros(velocity.shape, jnp.float32)
    laplace = jnp.zeros(velocity.shape, jnp.float32)
    for padded, direction, component in padded_list:
        gradient, curvature = stencil_terms(padded, direction, velocity.shape[direction])
        advect = advect + velocity[:, component:component + 1] * gradient
        laplace = laplace + curvature
    return (viscosity * laplace - advect).astype(jnp.bfloat16)


def one_snapshot(single):
    block = single[None]
    padded_wall = jnp.pad(block, ((0, 0), (0, 0), (2, 2), (0, 0), (0, 0)))
    padded_span = jnp.pad(block, ((0, 0), (0, 0), (0, 0), (2, 2), (0, 0)), mode="wrap")
    padded_stream = jnp.pad(block, ((0, 0), (0, 0), (0, 0), (0, 0), (2, 2)), mode="wrap")
    listed = ((padded_stream, 4, 0), (padded_wall, 2, 1), (padded_span, 3, 2))
    return feature_field(block.astype(jnp.float32), listed)[0]


def project(modes_flat, data_flat):
    return lax.dot_general(modes_flat, data_flat, (((1,), (1,)), ((), ())), preferred_element_type=jnp.float32)


def reference(snapshots, modes):
    features = lax.map(one_snapshot, snapshots)
    modes_flat = modes.reshape(modes.shape[0], -1)
    reduced_snapshots = project(modes_flat, snapshots.reshape(snapshots.shape[0], -1))
    reduced_features = project(modes_flat, features.reshape(features.shape[0], -1))
    high = lax.Precision.HIGHEST
    gram_snap = jnp.dot(reduced_snapshots, reduced_snapshots.T, precision=high, preferred_element_type=jnp.float32) / SNAPS
    gram_feature = jnp.dot(reduced_features, reduced_snapshots.T, precision=high, preferred_element_type=jnp.float32) / SNAPS
    products = jnp.dot(reduced_snapshots.T, reduced_snapshots, precision=high, preferred_element_type=jnp.float32) / MODES
    gram_quad = products * products
    return reduced_snapshots, reduced_features, gram_snap, gram_feature, gram_quad
```

```python
import functools

import jax
import jax.numpy as jnp
import numpy as np
from jax import lax
from jax.experimental import pallas as pl
from jax.experimental.pallas import tpu as pltpu
from jax.sharding import Mesh
from jax.sharding import PartitionSpec as P


GZ = ("gz_0", "gz_1")
BF16 = jnp.bfloat16
F32 = jnp.float32
VISCOSITY = 0.1
HIGH = lax.Precision.HIGHEST
NT = (((1,), (1,)), ((), ()))
TN = (((0,), (0,)), ((), ()))

GRAD = {-2: 1.0, -1: -8.0, 1: 8.0, 2: -1.0}
CURV = {-2: -1.0, -1: 16.0, 0: -30.0, 1: 16.0, 2: -1.0}


def plane_operator():
    op = np.zeros((192, 128), np.float32)

    def column(y, z):
        if y < 0:
            return 64 + (y + 2) * 8 + z
        if y > 7:
            return 80 + (y - 8) * 8 + z
        if z < 0:
            return 96 + y * 2 + z + 2
        if z > 7:
            return 112 + y * 2 + z - 8
        return y * 8 + z

    for y in range(8):
        for z in range(8):
            row = y * 8 + z
            for k, value in CURV.items():
                op[row, column(y + k, z)] += value
                op[row, column(y, z + k)] += value
            for k, value in GRAD.items():
                op[64 + row, column(y + k, z)] += value
                op[128 + row, column(y, z + k)] += value
    return op


def stream_operator():
    op = np.zeros((256, 256), np.float32)
    for part, taps in enumerate((GRAD, CURV)):
        for x in range(128):
            for k, value in taps.items():
                at = x + k
                if 0 <= at < 128:
                    op[at, part * 128 + x] += value
                else:
                    halo = at + 2 if at < 0 else at - 128 + 2
                    for j in range(32):
                        op[128 + 4 * j + halo, part * 128 + x] += value
    return op


def lane_masks():
    m, row, lane = np.meshgrid(np.arange(8), np.arange(64), np.arange(128), indexing="ij")
    return (lane // 4 == 4 * m + row // 16).astype(np.float32)


def lane_pick():
    op = np.zeros((128, 256), np.float32)
    for j in range(32):
        op[126, 4 * j] = op[127, 4 * j + 1] = 1
        op[0, 128 + 4 * j + 2] = op[1, 128 + 4 * j + 3] = 1
    return op


def span_pick():
    op = np.zeros((32, 64), np.float32)
    for y in range(8):
        for k in range(2):
            op[2 * y + k, 8 * y + k] = 1
            op[16 + 2 * y + k, 8 * y + 6 + k] = 1
    return op


def in_vmem(array):
    return pltpu.with_memory_space_constraint(array, pltpu.VMEM)


def any_space():
    return pl.BlockSpec(memory_space=pl.ANY)


def wall_pack(snap, first, count):
    def body(snap, low, high, sems):
        one = pltpu.make_async_copy(snap.at[pl.ds(first, count), pl.ds(0, 16)], low, sems.at[0])
        two = pltpu.make_async_copy(snap.at[pl.ds(first, count), pl.ds(48, 16)], high, sems.at[1])
        one.start()
        two.start()
        one.wait()
        two.wait()

    shape = pltpu.VMEM((count, 16, 128), BF16)
    vmem = pl.BlockSpec(memory_space=pltpu.VMEM)
    return pl.pallas_call(
        body,
        out_shape=(shape, shape),
        in_specs=[any_space()],
        out_specs=(vmem, vmem),
        scratch_shapes=[pltpu.SemaphoreType.DMA((2,))],
        name="wall_pack",
    )(snap)


def side_pack_body(snap, span, lanes, masks, low, high, right, left):
    for group in range(right.shape[0]):
        to_right = jnp.zeros((16, 128), F32)
        to_left = jnp.zeros((16, 128), F32)
        for pair in range(4):
            a = snap[8 * group + 2 * pair]
            b = snap[8 * group + 2 * pair + 1]
            picked = jnp.dot(span[...], jnp.concatenate([a, b], axis=1), preferred_element_type=F32).astype(BF16)
            for i in range(2):
                unit = 8 * group + 2 * pair + i
                low[unit] = picked[:16, 128 * i : 128 * (i + 1)]
                high[unit] = picked[16:, 128 * i : 128 * (i + 1)]
            ends = jnp.dot(jnp.concatenate([a, b], axis=0), lanes[...], preferred_element_type=F32)
            for i in range(2):
                for q in range(4):
                    rows = slice(64 * i + 16 * q, 64 * i + 16 * q + 16)
                    mask = masks[2 * pair + i, 16 * q : 16 * q + 16].astype(F32)
                    to_right += ends[rows, :128] * mask
                    to_left += ends[rows, 128:] * mask
        right[group] = to_right.astype(BF16)
        left[group] = to_left.astype(BF16)


def side_pack(snap, steps=4):
    units = snap.shape[0]
    n, g = units // steps, units // 8 // steps
    whole = lambda *shape: pl.BlockSpec(shape, lambda i: (0,) * len(shape))
    return pl.pallas_call(
        side_pack_body,
        grid=(steps,),
        out_shape=(
            jax.ShapeDtypeStruct((units, 16, 128), BF16),
            jax.ShapeDtypeStruct((units, 16, 128), BF16),
            jax.ShapeDtypeStruct((units // 8, 16, 128), BF16),
            jax.ShapeDtypeStruct((units // 8, 16, 128), BF16),
        ),
        in_specs=[
            pl.BlockSpec((n, 64, 128), lambda i: (i, 0, 0)),
            whole(32, 64),
            whole(128, 256),
            whole(8, 64, 128),
        ],
        out_specs=(
            pl.BlockSpec((n, 16, 128), lambda i: (i, 0, 0)),
            pl.BlockSpec((n, 16, 128), lambda i: (i, 0, 0)),
            pl.BlockSpec((g, 16, 128), lambda i: (i, 0, 0)),
            pl.BlockSpec((g, 16, 128), lambda i: (i, 0, 0)),
        ),
        name="side_pack",
    )(snap, jnp.asarray(span_pick(), BF16), jnp.asarray(lane_pick(), BF16), jnp.asarray(lane_masks(), BF16))


def same_span(total, count):
    rows = lax.broadcasted_iota(jnp.int32, total.shape, 0) % 8
    lanes = lax.broadcasted_iota(jnp.int32, total.shape, 1)
    kept = jnp.where(rows == lanes % 8, total, 0.0).reshape(128, 8, 8 * count).sum(axis=1)
    s = lax.broadcasted_iota(jnp.int32, (count, 8 * count), 0)
    at = lax.broadcasted_iota(jnp.int32, (count, 8 * count), 1)
    group = (at // 8 == s).astype(F32)
    return lax.dot_general(group, kept, NT, precision=HIGH, preferred_element_type=F32)


def project(modes, data, total):
    for k in range(12):
        a = jnp.concatenate([modes[2 * k].reshape(1024, 128), modes[2 * k + 1].reshape(1024, 128)], axis=1)
        b = jnp.concatenate([data[2 * k], data[2 * k + 1]], axis=1)
        part = lax.dot_general(a, b, NT, preferred_element_type=F32)
        if k == 0:
            total[...] = part
        else:
            total[...] += part


def snap_project_body(modes, snap, out, modes_in, snap_in, total, sems):
    copies = []
    for k in range(24):
        copies.append(pltpu.make_async_copy(modes.at[:, k], modes_in.at[k], sems.at[0, k]))
        copies.append(pltpu.make_async_copy(snap.at[:, k], snap_in.at[k], sems.at[1, k]))
    for c in copies:
        c.start()
    for c in copies:
        c.wait()

    class Rows:
        def __getitem__(self, k):
            return snap_in[k].reshape(512, 128)

    project(modes_in, Rows(), total)
    out[...] = same_span(total[...], 64)


def snap_project(modes, snap):
    return pl.pallas_call(
        snap_project_body,
        out_shape=jax.ShapeDtypeStruct((64, 128), F32),
        in_specs=[any_space(), any_space()],
        out_specs=pl.BlockSpec(memory_space=pltpu.VMEM),
        scratch_shapes=[
            pltpu.VMEM((24, 128, 8, 128), BF16),
            pltpu.VMEM((24, 64, 8, 128), BF16),
            pltpu.VMEM((1024, 512), F32),
            pltpu.SemaphoreType.DMA((2, 24)),
        ],
        name="snap_project",
    )(modes, snap)


def feature_body(
    first, modes, snap, y_low, y_high, z_low, z_high, x_low, x_high, plane, stream, masks, out, modes_in, field, total, sems
):
    step = pl.program_id(0)
    steps = pl.num_programs(0)
    copies = [pltpu.make_async_copy(modes.at[:, k], modes_in.at[k], sems.at[k]) for k in range(24)]

    @pl.when(step == 0)
    def _():
        for c in copies:
            c.start()

    count = snap.shape[0] // 3
    near = step * (3 * count)
    far = near + 3 * first
    x_at = pl.ds(far // 8, 3 * count // 8)
    x_halo = x_low[x_at] + x_high[x_at]
    for pair in range(count // 2):
        units = [[3 * (2 * pair + i) + c for c in range(3)] for i in range(2)]
        cells = [[snap[u] for u in row] for row in units]
        velocity = [[v.astype(F32) * (1.0 / 12.0) for v in row] for row in cells]
        along = []
        for i in range(2):
            inside = jnp.concatenate(cells[i], axis=0)
            beside = jnp.concatenate(
                [jnp.concatenate([x_halo[u // 8]] * 4, axis=0) * masks[u % 8] for u in units[i]], axis=0
            )
            along.append(
                jnp.dot(jnp.concatenate([inside, beside], axis=1), stream[...], preferred_element_type=F32)
            )
        for c in range(3):
            padded = [
                jnp.concatenate(
                    [cells[i][c], y_low[near + u], y_high[near + u], z_low[far + u], z_high[far + u]], axis=0
                )
                for i, u in ((0, units[0][c]), (1, units[1][c]))
            ]
            across = jnp.dot(plane[...], jnp.concatenate(padded, axis=1), preferred_element_type=F32)
            both = []
            for i in range(2):
                lanes = slice(128 * i, 128 * (i + 1))
                rows = slice(64 * c, 64 * (c + 1))
                laplace = across[0:64, lanes] + along[i][rows, 128:256]
                advect = (
                    velocity[i][0] * along[i][rows, 0:128]
                    + velocity[i][1] * across[64:128, lanes]
                    + velocity[i][2] * across[128:192, lanes]
                )
                both.append((laplace * (VISCOSITY / 12.0) - advect).reshape(8, 8, 128))
            stacked = jnp.concatenate(both, axis=1).astype(BF16)
            start = pl.multiple_of((step * count + 2 * pair) * 8, 16)
            field[8 * c : 8 * c + 8, pl.ds(start, 16), :] = stacked

    @pl.when(step == steps - 1)
    def _():
        for c in copies:
            c.wait()
        project(modes_in, field, total)
        out[...] = same_span(total[...], out.shape[0])


def feature_project(modes, snap, y_low, y_high, z_low, z_high, x_low, x_high, first, count, steps=4):
    n = 3 * count // steps
    off = 3 * first // n
    there = lambda *shape: pl.BlockSpec(shape, lambda i: (i + off,) + (0,) * (len(shape) - 1))
    whole = lambda *shape: pl.BlockSpec(shape, lambda i: (0,) * len(shape))
    resident = pl.BlockSpec(memory_space=pltpu.VMEM)
    return pl.pallas_call(
        functools.partial(feature_body, first),
        grid=(steps,),
        out_shape=jax.ShapeDtypeStruct((count, 128), F32),
        in_specs=[
            any_space(),
            there(n, 64, 128),
            resident,
            resident,
            resident,
            resident,
            resident,
            resident,
            whole(192, 128),
            whole(256, 256),
            whole(8, 64, 128),
        ],
        out_specs=whole(count, 128),
        scratch_shapes=[
            pltpu.VMEM((24, 128, 8, 128), BF16),
            pltpu.VMEM((24, 8 * count, 128), BF16),
            pltpu.VMEM((1024, 8 * count), F32),
            pltpu.SemaphoreType.DMA((24,)),
        ],
        name="feature_project",
    )(
        modes,
        snap,
        *map(in_vmem, (y_low, y_high, z_low, z_high, x_low, x_high)),
        jnp.asarray(plane_operator(), BF16),
        jnp.asarray(stream_operator(), BF16),
        jnp.asarray(lane_masks(), BF16),
    )


def gram_body(core, mine, other, snap_out, feature_out, gram_snap, gram_feature, gram_quad):
    first = core[0] == 0
    rs = jnp.where(first, mine[...], other[...])
    rf = jnp.where(first, other[...], mine[...])
    snap_out[...] = rs
    feature_out[...] = rf
    dot = functools.partial(lax.dot_general, precision=HIGH, preferred_element_type=F32)
    gram_snap[...] = dot(rs, rs, TN) * (1.0 / 64)
    gram_feature[...] = dot(rf, rs, TN) * (1.0 / 64)
    products = dot(rs, rs, NT) * (1.0 / 128)
    gram_quad[...] = products * products


def grams(core, mine, other):
    shape = lambda *s: jax.ShapeDtypeStruct(s, F32)
    vmem = pl.BlockSpec(memory_space=pltpu.VMEM)
    return pl.pallas_call(
        gram_body,
        in_specs=[pl.BlockSpec(memory_space=pltpu.SMEM), vmem, vmem],
        out_shape=(shape(64, 128), shape(64, 128), shape(128, 128), shape(128, 128), shape(64, 64)),
        name="grams",
    )(core, in_vmem(mine), in_vmem(other))


def shifted(value, axis, count, by, closed):
    pairs = [(i, (i + by) % count) for i in range(count) if closed or 0 <= i + by < count]
    return lax.ppermute(value, axis, pairs)


def swapped(value, axis, partners):
    return lax.ppermute(value, axis, list(enumerate(partners)))


ROUNDS = (
    ("gx", (1, 0, 3, 2)),
    ("gx", (3, 2, 1, 0)),
    ("gy", (1, 0, 3, 2)),
    ("gy", (3, 2, 1, 0)),
    ("gz_0", (1, 0, 3, 2, 5, 4, 7, 6)),
    ("gz_0", (2, 3, 0, 1, 6, 7, 4, 5)),
    ("gz_0", (6, 7, 4, 5, 2, 3, 0, 1)),
)
CHUNKS = ((0, 32), (32, 32))


def shards(snapshots, modes):
    units = snapshots.reshape(192, 64, 128)
    modes = modes.reshape(128, 24, 8, 128)
    walls = []
    for first, count in CHUNKS:
        low, high = wall_pack(units, 3 * first, 3 * count)
        up = shifted(high, "gy", 4, 1, False)
        down = shifted(low, "gy", 4, -1, False)
        walls.append((up, down))
    low, high, right, left = side_pack(units)
    z_low = shifted(high, GZ, 16, 1, True)
    z_high = shifted(low, GZ, 16, -1, True)
    x_low = shifted(right, "gx", 4, 1, True)
    x_high = shifted(left, "gx", 4, -1, True)
    parts = [snap_project(modes, snapshots.reshape(64, 24, 8, 128))]
    for (first, count), (y_low, y_high) in zip(CHUNKS, walls):
        parts.append(
            feature_project(modes, units, y_low, y_high, z_low, z_high, x_low, x_high, first, count)
        )
    core = lax.axis_index("gz_1")
    snap_part, feature_part = parts[0], jnp.concatenate(parts[1:], axis=0)
    mine = jnp.where(core == 0, snap_part, feature_part)
    total = mine + swapped(jnp.where(core == 0, feature_part, snap_part), "gz_1", (1, 0))
    for axis, partners in ROUNDS:
        total = total + swapped(total, axis, partners)
    rs, rf, gram_snap, gram_feature, gram_quad = grams(
        core.reshape(1).astype(jnp.int32), total, swapped(total, "gz_1", (1, 0))
    )
    return rs.T, rf.T, gram_snap, gram_feature, gram_quad


def solution(mesh):
    finer = Mesh(
        mesh.devices.reshape(mesh.shape["gx"], mesh.shape["gy"], 8, 2), ("gx", "gy", "gz_0", "gz_1")
    )
    placed = (P(None, None, "gy", GZ, "gx"), P(None, None, "gy", GZ, "gx"))

    return jax.shard_map(shards, mesh=finer, in_specs=placed, out_specs=(P(), P(), P(), P(), P()), check_vma=False)
```

```python
import functools

import jax
import jax.numpy as jnp
import numpy as np
from jax import lax
from jax.experimental import pallas as pl
from jax.experimental.pallas import tpu as pltpu
from jax.sharding import Mesh
from jax.sharding import PartitionSpec as P


GZ = ("gz_0", "gz_1")
BF16 = jnp.bfloat16
F32 = jnp.float32
VISCOSITY = 0.1
VMEM_LIMIT = 24 * 2**20
HIGH = lax.Precision.HIGHEST
NT = (((1,), (1,)), ((), ()))
TN = (((0,), (0,)), ((), ()))

GRAD = {-2: 1.0, -1: -8.0, 1: 8.0, 2: -1.0}
CURV = {-2: -1.0, -1: 16.0, 0: -30.0, 1: 16.0, 2: -1.0}


def span_operator():
    op = np.zeros((128, 96), np.float32)

    def column(y, z):
        if z < 0:
            return 64 + y * 2 + z + 2
        if z > 7:
            return 80 + y * 2 + z - 8
        return y * 8 + z

    for y in range(8):
        for z in range(8):
            row = y * 8 + z
            for k, value in CURV.items():
                op[row, column(y, z + k)] += value
                if 0 <= y + k < 8:
                    op[row, column(y + k, z)] += value
            for k, value in GRAD.items():
                op[64 + row, column(y, z + k)] += value
    return op


def stream_operator():
    op = np.zeros((256, 256), np.float32)
    for part, taps in enumerate((GRAD, CURV)):
        for x in range(128):
            for k, value in taps.items():
                at = x + k
                if 0 <= at < 128:
                    op[at, part * 128 + x] += value
                else:
                    halo = at + 2 if at < 0 else at - 128 + 2
                    for j in range(32):
                        op[128 + 4 * j + halo, part * 128 + x] += value
    return op


def lane_masks():
    m, row, lane = np.meshgrid(np.arange(8), np.arange(64), np.arange(128), indexing="ij")
    return (lane // 4 == 4 * m + row // 16).astype(np.float32)


def in_vmem(array):
    return pltpu.with_memory_space_constraint(array, pltpu.VMEM)


def from_hbm(array):
    return pltpu.with_memory_space_constraint(array, pltpu.HBM)


def in_hbm():
    return pl.BlockSpec(memory_space=pltpu.HBM)


def resident():
    return pl.BlockSpec(memory_space=pltpu.VMEM)


def wall_pack_body(snap, low, high, low_in, high_in, sems):
    ends = ((0, low, low_in), (48, high, high_in))
    reads = [pltpu.make_async_copy(snap.at[:, pl.ds(row, 16)], at, sems.at[i]) for i, (row, _, at) in enumerate(ends)]
    writes = [pltpu.make_async_copy(at, to, sems.at[2 + i]) for i, (_, to, at) in enumerate(ends)]
    for c in reads:
        c.start()
    for r, w in zip(reads, writes):
        r.wait()
        w.start()
    for w in writes:
        w.wait()


def wall_pack(snap):
    shape = jax.ShapeDtypeStruct((192, 16, 128), BF16)
    block = pltpu.VMEM((192, 16, 128), BF16)
    return pl.pallas_call(
        wall_pack_body,
        out_shape=(shape, shape),
        in_specs=[in_hbm()],
        out_specs=(in_hbm(), in_hbm()),
        scratch_shapes=[block, block, pltpu.SemaphoreType.DMA((4,))],
        compiler_params=pltpu.CompilerParams(vmem_limit_bytes=VMEM_LIMIT),
        name="wall_pack",
    )(from_hbm(snap))


def side_pack_body(snap, low, high, right, left):
    grid = lambda shape: [lax.broadcasted_iota(jnp.int32, shape, d) for d in range(2)]
    row, col = grid((32, 64))
    wanted = (row % 16) // 2 * 8 + row % 2 + jnp.where(row < 16, 0, 6)
    span = (col == wanted).astype(F32).astype(BF16)
    row, col = grid((128, 256))
    last = (col < 128) & (col % 4 < 2) & (row == 126 + col % 4)
    first = (col >= 128) & (col % 4 >= 2) & (row == col % 4 - 2)
    lanes = (last | first).astype(F32).astype(BF16)
    lane = lax.broadcasted_iota(jnp.int32, (16, 128), 1) // 4

    def group_of(group, _):
        units = [snap[8 * group + m] for m in range(8)]
        for pair in range(4):
            both = jnp.concatenate(units[2 * pair : 2 * pair + 2], axis=1)
            picked = jnp.dot(span, both, preferred_element_type=F32).astype(BF16)
            for i in range(2):
                low[8 * group + 2 * pair + i] = picked[:16, 128 * i : 128 * (i + 1)]
                high[8 * group + 2 * pair + i] = picked[16:, 128 * i : 128 * (i + 1)]
        ends = jnp.dot(jnp.concatenate(units, axis=0), lanes, preferred_element_type=F32)
        to_right = jnp.zeros((16, 128), F32)
        to_left = jnp.zeros((16, 128), F32)
        for j in range(32):
            to_right = jnp.where(lane == j, ends[16 * j : 16 * j + 16, :128], to_right)
            to_left = jnp.where(lane == j, ends[16 * j : 16 * j + 16, 128:], to_left)
        right[group] = to_right.astype(BF16)
        left[group] = to_left.astype(BF16)
        return _

    lax.fori_loop(0, 24, group_of, 0, unroll=4)


def side_pack(snap):
    wide, slim = jax.ShapeDtypeStruct((192, 16, 128), BF16), jax.ShapeDtypeStruct((24, 16, 128), BF16)
    return pl.pallas_call(
        side_pack_body,
        out_shape=(wide, wide, slim, slim),
        in_specs=[resident()],
        out_specs=(resident(),) * 4,
        compiler_params=pltpu.CompilerParams(vmem_limit_bytes=VMEM_LIMIT),
        name="side_pack",
    )(in_vmem(snap))


def same_span(total, out):
    lanes = lax.broadcasted_iota(jnp.int32, (128, 128), 1) % 8
    s = lax.broadcasted_iota(jnp.int32, (16, 128), 0)
    at = lax.broadcasted_iota(jnp.int32, (16, 128), 1)
    group = (at // 8 == s).astype(F32)
    for block in range(4):
        kept = total[block, pl.ds(0, 128, stride=8), :]
        for z in range(1, 8):
            kept = jnp.where(lanes == z, total[block, pl.ds(z, 128, stride=8), :], kept)
        out[16 * block : 16 * block + 16] = lax.dot_general(
            group, kept, NT, precision=HIGH, preferred_element_type=F32
        )


def add_products(modes, planes, data, total, base):
    a = jnp.concatenate([modes[k].reshape(1024, 128) for k in planes], axis=1)
    part = lax.dot_general(a, jnp.concatenate(data, axis=1), NT, preferred_element_type=F32)
    for block in range(4):
        lanes = part[:, 128 * block : 128 * block + 128]
        total[block] = lanes if base is None else base[block] + lanes


def snap_project_body(modes, snap, out, modes_in, snap_in, total, sems):
    copies = []
    for k in range(24):
        copies.append(pltpu.make_async_copy(modes.at[:, k], modes_in.at[k], sems.at[0, k]))
        copies.append(pltpu.make_async_copy(snap.at[:, k], snap_in.at[k], sems.at[1, k]))
    for c in copies:
        c.start()
    for k in range(0, 24, 4):
        for c in copies[2 * k : 2 * k + 8]:
            c.wait()
        planes = range(k, k + 4)
        add_products(modes_in, planes, [snap_in[p].reshape(512, 128) for p in planes], total, total if k else None)
    same_span(total, out)


def snap_project(modes, snap):
    return pl.pallas_call(
        snap_project_body,
        out_shape=(jax.ShapeDtypeStruct((64, 128), F32), jax.ShapeDtypeStruct((24, 128, 8, 128), BF16)),
        in_specs=[in_hbm(), in_hbm()],
        out_specs=(resident(), resident()),
        scratch_shapes=[
            pltpu.VMEM((24, 64, 8, 128), BF16),
            pltpu.VMEM((4, 1024, 128), F32),
            pltpu.SemaphoreType.DMA((2, 24)),
        ],
        compiler_params=pltpu.CompilerParams(vmem_limit_bytes=VMEM_LIMIT),
        name="snap_project",
    )(from_hbm(modes), from_hbm(snap))


def feature_body(
    modes_in, snap, z_low, z_high, x_low, x_high, span, stream, masks, total, edges, field
):
    def block(step, _):
        for pair in range(4):
            base = 24 * step + 6 * pair
            units = [[6 * pair + 3 * i + c for c in range(3)] for i in range(2)]
            cells = [[snap[base + 3 * i + c] for c in range(3)] for i in range(2)]
            inside = jnp.concatenate(cells[0] + cells[1], axis=0)
            beside = []
            for u in units[0] + units[1]:
                halo = x_low[3 * step + u // 8] + x_high[3 * step + u // 8]
                beside.append(jnp.concatenate([halo] * 4, axis=0) * masks[u % 8])
            beside = jnp.concatenate(beside, axis=0)
            along = jnp.dot(jnp.concatenate([inside, beside], axis=1), stream[...], preferred_element_type=F32)
            wide = [[v.astype(F32).reshape(8, 8, 128) for v in row] for row in cells]
            velocity = [[v * (1.0 / 12.0) for v in row] for row in wide]
            for c in range(3):
                padded = [
                    jnp.concatenate(
                        [cells[i][c], z_low[base + 3 * i + c], z_high[base + 3 * i + c]], axis=0
                    )
                    for i in range(2)
                ]
                across = jnp.dot(span[...], jnp.concatenate(padded, axis=1), preferred_element_type=F32)
                both = []
                for i in range(2):
                    none = jnp.zeros((2, 8, 128), F32)
                    ext = jnp.concatenate([none, wide[i][c], none], axis=0)
                    near, far = ext[3:11] - ext[1:9], ext[4:12] - ext[0:8]
                    lanes = slice(128 * i, 128 * (i + 1))
                    rows = slice(192 * i + 64 * c, 192 * i + 64 * (c + 1))
                    cube = lambda part: part.reshape(8, 8, 128)
                    laplace = cube(across[0:64, lanes]) + cube(along[rows, 128:256])
                    advect = (
                        velocity[i][0] * cube(along[rows, 0:128])
                        + velocity[i][1] * (8.0 * near - far)
                        + velocity[i][2] * cube(across[64:128, lanes])
                    )
                    value = laplace * (VISCOSITY / 12.0) - advect
                    both.append(value[2:6])
                    edges[base + 3 * i + c, 0:2] = value[0:2]
                    edges[base + 3 * i + c, 2:4] = value[6:8]
                start = pl.multiple_of((8 * step + 2 * pair) * 8, 16)
                field[4 * c : 4 * c + 4, pl.ds(start, 16), :] = jnp.concatenate(both, axis=1).astype(BF16)
        return _

    lax.fori_loop(0, 8, block, 0)
    for c in range(3):
        planes = range(8 * c + 2, 8 * c + 6)
        add_products(modes_in, planes, [field[4 * c + k] for k in range(4)], total, total if c else None)


def feature_project(modes_in, snap, z_low, z_high, x_low, x_high):
    consts = [jnp.asarray(v, BF16) for v in (span_operator(), stream_operator(), lane_masks())]
    return pl.pallas_call(
        feature_body,
        out_shape=(
            jax.ShapeDtypeStruct((4, 1024, 128), F32),
            jax.ShapeDtypeStruct((192, 4, 8, 128), F32),
        ),
        in_specs=[resident()] * 9,
        out_specs=(resident(), resident()),
        scratch_shapes=[pltpu.VMEM((12, 512, 128), BF16)],
        compiler_params=pltpu.CompilerParams(vmem_limit_bytes=VMEM_LIMIT),
        name="feature_project",
    )(*map(in_vmem, (modes_in, snap, z_low, z_high, x_low, x_high)), *consts)


def edge_body(modes_in, snap, edges, y_low, y_high, inner, out, field, total):
    k = VISCOSITY / 12.0

    def block(step, _):
        base = 12 * step
        values = []
        for i in range(4):
            wall = snap[base + 3 * i + 1].astype(F32) * (1.0 / 12.0)
            wall = wall.reshape(8, 8, 128)
            below_near, below_far = 16.0 * k + 8.0 * wall[0], k + wall[0]
            above_near, above_far = 16.0 * k - 8.0 * wall[7], k - wall[7]
            second, seventh = k + wall[1], k - wall[6]
            row = []
            for c in range(3):
                u = base + 3 * i + c
                below = y_low[u].astype(F32).reshape(2, 8, 128)
                above = y_high[u].astype(F32).reshape(2, 8, 128)
                value = edges[u]
                row.append(
                    jnp.stack(
                        [
                            value[0] + (below_near * below[1] - below_far * below[0]),
                            value[1] - second * below[1],
                            value[2] - seventh * above[0],
                            value[3] + (above_near * above[0] - above_far * above[1]),
                        ]
                    )
                )
            values.append(row)
        for pair in range(2):
            start = pl.multiple_of((4 * step + 2 * pair) * 8, 16)
            for c in range(3):
                both = jnp.concatenate([values[2 * pair][c], values[2 * pair + 1][c]], axis=1)
                field[4 * c : 4 * c + 4, pl.ds(start, 16), :] = both.astype(BF16)
        return _

    lax.fori_loop(0, 16, block, 0, unroll=4)
    for c in range(3):
        planes = [8 * c, 8 * c + 1, 8 * c + 6, 8 * c + 7]
        add_products(modes_in, planes, [field[4 * c + p] for p in range(4)], total, total if c else inner)
    same_span(total, out)


def edge_project(modes_in, snap, edges, y_low, y_high, inner):
    return pl.pallas_call(
        edge_body,
        out_shape=jax.ShapeDtypeStruct((64, 128), F32),
        in_specs=[resident()] * 6,
        out_specs=resident(),
        scratch_shapes=[pltpu.VMEM((12, 512, 128), BF16), pltpu.VMEM((4, 1024, 128), F32)],
        compiler_params=pltpu.CompilerParams(vmem_limit_bytes=VMEM_LIMIT),
        name="edge_project",
    )(*map(in_vmem, (modes_in, snap, edges, y_low, y_high, inner)))


def gram_body(core, mine, other, snap_out, feature_out, gram_snap, gram_feature, gram_quad):
    first = core[0] == 0
    rs = jnp.where(first, mine[...], other[...])
    rf = jnp.where(first, other[...], mine[...])
    snap_out[...] = rs
    feature_out[...] = rf
    dot = functools.partial(lax.dot_general, precision=HIGH, preferred_element_type=F32)
    gram_snap[...] = dot(rs, rs, TN) * (1.0 / 64)
    gram_feature[...] = dot(rf, rs, TN) * (1.0 / 64)
    products = dot(rs, rs, NT) * (1.0 / 128)
    gram_quad[...] = products * products


def grams(core, mine, other):
    shape = lambda *s: jax.ShapeDtypeStruct(s, F32)
    vmem = pl.BlockSpec(memory_space=pltpu.VMEM)
    return pl.pallas_call(
        gram_body,
        in_specs=[pl.BlockSpec(memory_space=pltpu.SMEM), vmem, vmem],
        out_shape=(shape(64, 128), shape(64, 128), shape(128, 128), shape(128, 128), shape(64, 64)),
        compiler_params=pltpu.CompilerParams(vmem_limit_bytes=VMEM_LIMIT),
        name="grams",
    )(core, in_vmem(mine), in_vmem(other))


def shifted(value, axis, count, by, closed):
    pairs = [(i, (i + by) % count) for i in range(count) if closed or 0 <= i + by < count]
    return lax.ppermute(value, axis, pairs)


def swapped(value, axis, partners):
    return lax.ppermute(value, axis, list(enumerate(partners)))


ROUNDS = (
    ("gx", (1, 0, 3, 2)),
    ("gx", (3, 2, 1, 0)),
    ("gy", (1, 0, 3, 2)),
    ("gy", (3, 2, 1, 0)),
    ("gz_0", (1, 0, 3, 2, 5, 4, 7, 6)),
    ("gz_0", (2, 3, 0, 1, 6, 7, 4, 5)),
    ("gz_0", (6, 7, 4, 5, 2, 3, 0, 1)),
)


def shards(snapshots, modes):
    units = snapshots.reshape(192, 64, 128)
    low, high = wall_pack(units)
    y_low = shifted(high, "gy", 4, 1, False)
    y_high = shifted(low, "gy", 4, -1, False)
    low, high, right, left = side_pack(units)
    z_low = shifted(high, GZ, 16, 1, True)
    z_high = shifted(low, GZ, 16, -1, True)
    x_low = shifted(right, "gx", 4, 1, True)
    x_high = shifted(left, "gx", 4, -1, True)
    snap_part, modes_in = snap_project(modes.reshape(128, 24, 8, 128), snapshots.reshape(64, 24, 8, 128))
    inner, edges = feature_project(modes_in, units, z_low, z_high, x_low, x_high)
    feature_part = edge_project(modes_in, units, edges, y_low, y_high, inner)
    core = lax.axis_index("gz_1")
    mine = jnp.where(core == 0, snap_part, feature_part)
    total = mine + swapped(jnp.where(core == 0, feature_part, snap_part), "gz_1", (1, 0))
    for axis, partners in ROUNDS:
        total = total + swapped(total, axis, partners)
    rs, rf, gram_snap, gram_feature, gram_quad = grams(
        core.reshape(1).astype(jnp.int32), total, swapped(total, "gz_1", (1, 0))
    )
    return rs.T, rf.T, gram_snap, gram_feature, gram_quad


def solution(mesh):
    finer = Mesh(
        mesh.devices.reshape(mesh.shape["gx"], mesh.shape["gy"], 8, 2), ("gx", "gy", "gz_0", "gz_1")
    )
    placed = (P(None, None, "gy", GZ, "gx"), P(None, None, "gy", GZ, "gx"))

    return jax.shard_map(shards, mesh=finer, in_specs=placed, out_specs=(P(), P(), P(), P(), P()), check_vma=False)
```

```python
import functools

import jax
import jax.numpy as jnp
import numpy as np
from jax import lax
from jax.experimental import pallas as pl
from jax.experimental.pallas import tpu as pltpu
from jax.sharding import Mesh
from jax.sharding import PartitionSpec as P


GZ = ("gz_0", "gz_1")
BF16 = jnp.bfloat16
F32 = jnp.float32
VISCOSITY = 0.1
VMEM_LIMIT = 24 * 2**20
HIGH = lax.Precision.HIGHEST
NT = (((1,), (1,)), ((), ()))
TN = (((0,), (0,)), ((), ()))

GRAD = {-2: 1.0, -1: -8.0, 1: 8.0, 2: -1.0}
CURV = {-2: -1.0, -1: 16.0, 0: -30.0, 1: 16.0, 2: -1.0}


def span_operator():
    op = np.zeros((128, 96), np.float32)

    def column(y, z):
        if z < 0:
            return 64 + y * 2 + z + 2
        if z > 7:
            return 80 + y * 2 + z - 8
        return y * 8 + z

    for y in range(8):
        for z in range(8):
            row = y * 8 + z
            for k, value in CURV.items():
                op[row, column(y, z + k)] += value
                if 0 <= y + k < 8:
                    op[row, column(y + k, z)] += value
            for k, value in GRAD.items():
                op[64 + row, column(y, z + k)] += value
    return op


def stream_operator():
    op = np.zeros((256, 256), np.float32)
    for part, taps in enumerate((GRAD, CURV)):
        for x in range(128):
            for k, value in taps.items():
                at = x + k
                if 0 <= at < 128:
                    op[at, part * 128 + x] += value
                else:
                    halo = at + 2 if at < 0 else at - 128 + 2
                    for j in range(32):
                        op[128 + 4 * j + halo, part * 128 + x] += value
    return op


def lane_masks():
    m, row, lane = np.meshgrid(np.arange(8), np.arange(64), np.arange(128), indexing="ij")
    return (lane // 4 == 4 * m + row // 16).astype(np.float32)


def in_vmem(array):
    return pltpu.with_memory_space_constraint(array, pltpu.VMEM)


def from_hbm(array):
    return pltpu.with_memory_space_constraint(array, pltpu.HBM)


def in_hbm():
    return pl.BlockSpec(memory_space=pltpu.HBM)


def resident():
    return pl.BlockSpec(memory_space=pltpu.VMEM)


def wall_pack_body(snap, low, high, units, sems):
    parts = (pl.ds(0, 16), pl.ds(48, 16), pl.ds(16, 32))
    reads = [pltpu.make_async_copy(snap.at[:, at], units.at[:, at], sems.at[i]) for i, at in enumerate(parts)]
    writes = [
        pltpu.make_async_copy(units.at[:, at], to, sems.at[3 + i]) for i, (at, to) in enumerate(zip(parts, (low, high)))
    ]
    for c in reads:
        c.start()
    for r, w in zip(reads, writes):
        r.wait()
        w.start()
    reads[2].wait()
    for w in writes:
        w.wait()


def wall_pack(snap):
    shape = jax.ShapeDtypeStruct((192, 16, 128), BF16)
    return pl.pallas_call(
        wall_pack_body,
        out_shape=(shape, shape, jax.ShapeDtypeStruct((192, 64, 128), BF16)),
        in_specs=[in_hbm()],
        out_specs=(in_hbm(), in_hbm(), resident()),
        scratch_shapes=[pltpu.SemaphoreType.DMA((5,))],
        compiler_params=pltpu.CompilerParams(vmem_limit_bytes=VMEM_LIMIT),
        name="wall_pack",
    )(from_hbm(snap))


def side_pack_body(snap, low, high, right, left):
    grid = lambda shape: [lax.broadcasted_iota(jnp.int32, shape, d) for d in range(2)]
    row, col = grid((32, 64))
    wanted = (row % 16) // 2 * 8 + row % 2 + jnp.where(row < 16, 0, 6)
    span = (col == wanted).astype(F32).astype(BF16)
    row, col = grid((128, 256))
    last = (col < 128) & (col % 4 < 2) & (row == 126 + col % 4)
    first = (col >= 128) & (col % 4 >= 2) & (row == col % 4 - 2)
    lanes = (last | first).astype(F32).astype(BF16)
    lane = lax.broadcasted_iota(jnp.int32, (16, 128), 1) // 4

    def group_of(group, _):
        units = [snap[8 * group + m] for m in range(8)]
        for pair in range(4):
            both = jnp.concatenate(units[2 * pair : 2 * pair + 2], axis=1)
            picked = jnp.dot(span, both, preferred_element_type=F32).astype(BF16)
            for i in range(2):
                low[8 * group + 2 * pair + i] = picked[:16, 128 * i : 128 * (i + 1)]
                high[8 * group + 2 * pair + i] = picked[16:, 128 * i : 128 * (i + 1)]
        ends = jnp.dot(jnp.concatenate(units, axis=0), lanes, preferred_element_type=F32)
        to_right = jnp.zeros((16, 128), F32)
        to_left = jnp.zeros((16, 128), F32)
        for j in range(32):
            to_right = jnp.where(lane == j, ends[16 * j : 16 * j + 16, :128], to_right)
            to_left = jnp.where(lane == j, ends[16 * j : 16 * j + 16, 128:], to_left)
        right[group] = to_right.astype(BF16)
        left[group] = to_left.astype(BF16)
        return _

    lax.fori_loop(0, 24, group_of, 0, unroll=4)


def side_pack(snap):
    wide, slim = jax.ShapeDtypeStruct((192, 16, 128), BF16), jax.ShapeDtypeStruct((24, 16, 128), BF16)
    return pl.pallas_call(
        side_pack_body,
        out_shape=(wide, wide, slim, slim),
        in_specs=[resident()],
        out_specs=(resident(),) * 4,
        compiler_params=pltpu.CompilerParams(vmem_limit_bytes=VMEM_LIMIT),
        name="side_pack",
    )(in_vmem(snap))


def same_span(total, half, out):
    lanes = lax.broadcasted_iota(jnp.int32, (64, 128), 1) % 8
    s = lax.broadcasted_iota(jnp.int32, (16, 128), 0)
    at = lax.broadcasted_iota(jnp.int32, (16, 128), 1)
    group = (at // 8 == s).astype(F32)
    for block in range(4):
        kept = total[block, pl.ds(512 * half, 64, stride=8), :]
        for z in range(1, 8):
            kept = jnp.where(lanes == z, total[block, pl.ds(512 * half + z, 64, stride=8), :], kept)
        out[16 * block : 16 * block + 16, 64 * half : 64 * half + 64] = lax.dot_general(
            group, kept, NT, precision=HIGH, preferred_element_type=F32
        )


def add_products(modes, half, planes, data, total, base):
    a = jnp.concatenate([modes[k, 64 * half : 64 * half + 64].reshape(512, 128) for k in planes], axis=1)
    part = lax.dot_general(a, jnp.concatenate(data, axis=1), NT, preferred_element_type=F32)
    rows = slice(512 * half, 512 * half + 512)
    for block in range(4):
        lanes = part[:, 128 * block : 128 * block + 128]
        total[block, rows] = lanes if base is None else base[block, rows] + lanes


def snap_project_body(modes, snap, out, modes_in, snap_in, total, sems):
    copies = []
    for k in range(24):
        copies.append(pltpu.make_async_copy(modes.at[:, k], modes_in.at[k], sems.at[0, k]))
        copies.append(pltpu.make_async_copy(snap.at[:, k], snap_in.at[k], sems.at[1, k]))
    for c in copies:
        c.start()
    for half, size in ((0, 6), (1, 12)):
        for k in range(0, 24, size):
            if half == 0:
                for c in copies[2 * k : 2 * (k + size)]:
                    c.wait()
            planes = range(k, k + size)
            data = [snap_in[p].reshape(512, 128) for p in planes]
            add_products(modes_in, half, planes, data, total, total if k else None)
        same_span(total, half, out)


def snap_project(modes, snap):
    return pl.pallas_call(
        snap_project_body,
        out_shape=(jax.ShapeDtypeStruct((64, 128), F32), jax.ShapeDtypeStruct((24, 128, 8, 128), BF16)),
        in_specs=[in_hbm(), in_hbm()],
        out_specs=(resident(), resident()),
        scratch_shapes=[
            pltpu.VMEM((24, 64, 8, 128), BF16),
            pltpu.VMEM((4, 1024, 128), F32),
            pltpu.SemaphoreType.DMA((2, 24)),
        ],
        compiler_params=pltpu.CompilerParams(vmem_limit_bytes=VMEM_LIMIT),
        name="snap_project",
    )(from_hbm(modes), from_hbm(snap))


def feature_body(
    modes_in, snap, z_low, z_high, x_low, x_high, span, stream, masks, total, edges, field
):
    def block(step, _):
        for pair in range(4):
            base = 24 * step + 6 * pair
            units = [[6 * pair + 3 * i + c for c in range(3)] for i in range(2)]
            cells = [[snap[base + 3 * i + c] for c in range(3)] for i in range(2)]
            inside = jnp.concatenate(cells[0] + cells[1], axis=0)
            beside = []
            for u in units[0] + units[1]:
                halo = x_low[3 * step + u // 8] + x_high[3 * step + u // 8]
                beside.append(jnp.concatenate([halo] * 4, axis=0) * masks[u % 8])
            beside = jnp.concatenate(beside, axis=0)
            along = jnp.dot(jnp.concatenate([inside, beside], axis=1), stream[...], preferred_element_type=F32)
            wide = [[v.astype(F32).reshape(8, 8, 128) for v in row] for row in cells]
            velocity = [[v * (1.0 / 12.0) for v in row] for row in wide]
            for c in range(3):
                padded = [
                    jnp.concatenate(
                        [cells[i][c], z_low[base + 3 * i + c], z_high[base + 3 * i + c]], axis=0
                    )
                    for i in range(2)
                ]
                across = jnp.dot(span[...], jnp.concatenate(padded, axis=1), preferred_element_type=F32)
                both = []
                for i in range(2):
                    none = jnp.zeros((2, 8, 128), F32)
                    ext = jnp.concatenate([none, wide[i][c], none], axis=0)
                    near, far = ext[3:11] - ext[1:9], ext[4:12] - ext[0:8]
                    lanes = slice(128 * i, 128 * (i + 1))
                    rows = slice(192 * i + 64 * c, 192 * i + 64 * (c + 1))
                    cube = lambda part: part.reshape(8, 8, 128)
                    laplace = cube(across[0:64, lanes]) + cube(along[rows, 128:256])
                    advect = (
                        velocity[i][0] * cube(along[rows, 0:128])
                        + velocity[i][1] * (8.0 * near - far)
                        + velocity[i][2] * cube(across[64:128, lanes])
                    )
                    value = laplace * (VISCOSITY / 12.0) - advect
                    both.append(value[2:6])
                    edges[base + 3 * i + c, 0:2] = value[0:2]
                    edges[base + 3 * i + c, 2:4] = value[6:8]
                start = pl.multiple_of((8 * step + 2 * pair) * 8, 16)
                field[4 * c : 4 * c + 4, pl.ds(start, 16), :] = jnp.concatenate(both, axis=1).astype(BF16)
        return _

    lax.fori_loop(0, 8, block, 0)
    planes = [8 * c + y for c in range(3) for y in range(2, 6)]
    for half in range(2):
        add_products(modes_in, half, planes, [field[k] for k in range(12)], total, None)


def feature_project(modes_in, snap, z_low, z_high, x_low, x_high):
    consts = [jnp.asarray(v, BF16) for v in (span_operator(), stream_operator(), lane_masks())]
    return pl.pallas_call(
        feature_body,
        out_shape=(
            jax.ShapeDtypeStruct((4, 1024, 128), F32),
            jax.ShapeDtypeStruct((192, 4, 8, 128), F32),
        ),
        in_specs=[resident()] * 9,
        out_specs=(resident(), resident()),
        scratch_shapes=[pltpu.VMEM((12, 512, 128), BF16)],
        compiler_params=pltpu.CompilerParams(vmem_limit_bytes=VMEM_LIMIT),
        name="feature_project",
    )(*map(in_vmem, (modes_in, snap, z_low, z_high, x_low, x_high)), *consts)


def edge_body(modes_in, snap, edges, y_low, y_high, inner, out, field, total):
    k = VISCOSITY / 12.0
    row = lax.axis_index("gy")
    has_below, has_above = row > 0, row < 3

    def block(step, _):
        base = 12 * step
        values = []
        for i in range(4):
            wall = snap[base + 3 * i + 1].astype(F32) * (1.0 / 12.0)
            wall = wall.reshape(8, 8, 128)
            below_near, below_far = 16.0 * k + 8.0 * wall[0], k + wall[0]
            above_near, above_far = 16.0 * k - 8.0 * wall[7], k - wall[7]
            second, seventh = k + wall[1], k - wall[6]
            row = []
            for c in range(3):
                u = base + 3 * i + c
                below = jnp.where(has_below, y_low[u].astype(F32), 0.0).reshape(2, 8, 128)
                above = jnp.where(has_above, y_high[u].astype(F32), 0.0).reshape(2, 8, 128)
                value = edges[u]
                row.append(
                    jnp.stack(
                        [
                            value[0] + (below_near * below[1] - below_far * below[0]),
                            value[1] - second * below[1],
                            value[2] - seventh * above[0],
                            value[3] + (above_near * above[0] - above_far * above[1]),
                        ]
                    )
                )
            values.append(row)
        for pair in range(2):
            start = pl.multiple_of((4 * step + 2 * pair) * 8, 16)
            for c in range(3):
                both = jnp.concatenate([values[2 * pair][c], values[2 * pair + 1][c]], axis=1)
                field[4 * c : 4 * c + 4, pl.ds(start, 16), :] = both.astype(BF16)
        return _

    lax.fori_loop(0, 16, block, 0, unroll=4)
    planes = [8 * c + y for c in range(3) for y in (0, 1, 6, 7)]
    for half in range(2):
        add_products(modes_in, half, planes, [field[k] for k in range(12)], total, inner)
        same_span(total, half, out)


def edge_project(modes_in, snap, edges, y_low, y_high, inner):
    return pl.pallas_call(
        edge_body,
        out_shape=jax.ShapeDtypeStruct((64, 128), F32),
        in_specs=[resident()] * 6,
        out_specs=resident(),
        scratch_shapes=[pltpu.VMEM((12, 512, 128), BF16), pltpu.VMEM((4, 1024, 128), F32)],
        compiler_params=pltpu.CompilerParams(vmem_limit_bytes=VMEM_LIMIT),
        name="edge_project",
    )(*map(in_vmem, (modes_in, snap, edges, y_low, y_high, inner)))


def gram_body(mine, other, snap_out, feature_out, gram_snap, gram_feature, gram_quad):
    first = lax.axis_index("gz_1") == 0
    rs = jnp.where(first, mine[...], other[...])
    rf = jnp.where(first, other[...], mine[...])
    snap_out[...] = rs
    feature_out[...] = rf
    dot = functools.partial(lax.dot_general, precision=HIGH, preferred_element_type=F32)
    gram_snap[...] = dot(rs, rs, TN) * (1.0 / 64)
    gram_feature[...] = dot(rf, rs, TN) * (1.0 / 64)
    products = dot(rs, rs, NT) * (1.0 / 128)
    gram_quad[...] = products * products


def grams(mine, other):
    shape = lambda *s: jax.ShapeDtypeStruct(s, F32)
    vmem = pl.BlockSpec(memory_space=pltpu.VMEM)
    return pl.pallas_call(
        gram_body,
        in_specs=[vmem, vmem],
        out_shape=(shape(64, 128), shape(64, 128), shape(128, 128), shape(128, 128), shape(64, 64)),
        compiler_params=pltpu.CompilerParams(vmem_limit_bytes=VMEM_LIMIT),
        name="grams",
    )(in_vmem(mine), in_vmem(other))


def shifted(value, axis, count, by):
    return lax.ppermute(value, axis, [(i, (i + by) % count) for i in range(count)])


def swapped(value, axis, partners):
    return lax.ppermute(value, axis, list(enumerate(partners)))


def other_core(value):
    return lax.ppermute(value, "gz_1", [(0, 1), (1, 0)])


ROUNDS = (
    ("gx", (1, 0, 3, 2)),
    ("gx", (3, 2, 1, 0)),
    ("gy", (1, 0, 3, 2)),
    ("gy", (3, 2, 1, 0)),
    ("gz_0", (1, 0, 3, 2, 5, 4, 7, 6)),
    ("gz_0", (2, 3, 0, 1, 6, 7, 4, 5)),
    ("gz_0", (6, 7, 4, 5, 2, 3, 0, 1)),
)


def shards(snapshots, modes):
    low, high, units = wall_pack(snapshots.reshape(192, 64, 128))
    y_low = shifted(high, "gy", 4, 1)
    y_high = shifted(low, "gy", 4, -1)
    low, high, right, left = side_pack(units)
    z_low = shifted(high, GZ, 16, 1)
    z_high = shifted(low, GZ, 16, -1)
    x_low = shifted(right, "gx", 4, 1)
    x_high = shifted(left, "gx", 4, -1)
    snap_part, modes_in = snap_project(modes.reshape(128, 24, 8, 128), snapshots.reshape(64, 24, 8, 128))
    inner, edges = feature_project(modes_in, units, z_low, z_high, x_low, x_high)
    feature_part = edge_project(modes_in, units, edges, y_low, y_high, inner)
    core = lax.axis_index("gz_1")
    mine = jnp.where(core == 0, snap_part, feature_part)
    total = mine + other_core(jnp.where(core == 0, feature_part, snap_part))
    for axis, partners in ROUNDS:
        total = total + swapped(total, axis, partners)
    rs, rf, gram_snap, gram_feature, gram_quad = grams(total, other_core(total))
    return rs.T, rf.T, gram_snap, gram_feature, gram_quad


def solution(mesh):
    finer = Mesh(
        mesh.devices.reshape(mesh.shape["gx"], mesh.shape["gy"], 8, 2), ("gx", "gy", "gz_0", "gz_1")
    )
    placed = (P(None, None, "gy", GZ, "gx"), P(None, None, "gy", GZ, "gx"))

    return jax.shard_map(shards, mesh=finer, in_specs=placed, out_specs=(P(), P(), P(), P(), P()), check_vma=False)
```

```python
import functools

import jax
import jax.numpy as jnp
import numpy as np
from jax import lax
from jax.experimental import pallas as pl
from jax.experimental.pallas import tpu as pltpu
from jax.sharding import Mesh
from jax.sharding import PartitionSpec as P


GZ = ("gz_0", "gz_1")
BF16 = jnp.bfloat16
F32 = jnp.float32
VISCOSITY = 0.1
VMEM_LIMIT = 10 * 2**20
HIGH = lax.Precision.HIGHEST
NT = (((1,), (1,)), ((), ()))
TN = (((0,), (0,)), ((), ()))

GRAD = {-2: 1.0, -1: -8.0, 1: 8.0, 2: -1.0}
CURV = {-2: -1.0, -1: 16.0, 0: -30.0, 1: 16.0, 2: -1.0}


def span_operator():
    op = np.zeros((128, 96), np.float32)

    def column(y, z):
        if z < 0:
            return 64 + y * 2 + z + 2
        if z > 7:
            return 80 + y * 2 + z - 8
        return y * 8 + z

    for y in range(8):
        for z in range(8):
            row = y * 8 + z
            for k, value in CURV.items():
                op[row, column(y, z + k)] += value
                if 0 <= y + k < 8:
                    op[row, column(y + k, z)] += value
            for k, value in GRAD.items():
                op[64 + row, column(y, z + k)] += value
    return op


def stream_operator():
    op = np.zeros((256, 256), np.float32)
    for part, taps in enumerate((GRAD, CURV)):
        for x in range(128):
            for k, value in taps.items():
                at = x + k
                if 0 <= at < 128:
                    op[at, part * 128 + x] += value
                else:
                    halo = at + 2 if at < 0 else at - 128 + 2
                    for j in range(32):
                        op[128 + 4 * j + halo, part * 128 + x] += value
    return op


def lane_masks():
    m, row, lane = np.meshgrid(np.arange(8), np.arange(64), np.arange(128), indexing="ij")
    return (lane // 4 == 4 * m + row // 16).astype(np.float32)


def in_vmem(array):
    return pltpu.with_memory_space_constraint(array, pltpu.VMEM)


def from_hbm(array):
    return pltpu.with_memory_space_constraint(array, pltpu.HBM)


def in_hbm():
    return pl.BlockSpec(memory_space=pltpu.HBM)


def resident():
    return pl.BlockSpec(memory_space=pltpu.VMEM)


def wall_pack_body(snap, low, high, units, sems):
    parts = (pl.ds(0, 16), pl.ds(48, 16), pl.ds(16, 32))
    reads = [pltpu.make_async_copy(snap.at[:, at], units.at[:, at], sems.at[i]) for i, at in enumerate(parts)]
    writes = [
        pltpu.make_async_copy(units.at[:, at], to, sems.at[3 + i]) for i, (at, to) in enumerate(zip(parts, (low, high)))
    ]
    for c in reads:
        c.start()
    for r, w in zip(reads, writes):
        r.wait()
        w.start()
    reads[2].wait()
    for w in writes:
        w.wait()


def wall_pack(snap):
    shape = jax.ShapeDtypeStruct((192, 16, 128), BF16)
    return pl.pallas_call(
        wall_pack_body,
        out_shape=(shape, shape, jax.ShapeDtypeStruct((192, 64, 128), BF16)),
        in_specs=[in_hbm()],
        out_specs=(in_hbm(), in_hbm(), resident()),
        scratch_shapes=[pltpu.SemaphoreType.DMA((5,))],
        compiler_params=pltpu.CompilerParams(vmem_limit_bytes=VMEM_LIMIT),
        name="wall_pack",
    )(from_hbm(snap))


def side_pack_body(snap, modes_hbm, snap_hbm, low, high, right, left, modes_in, snap_in, sems):
    copies = []
    for k in range(24):
        copies.append(pltpu.make_async_copy(modes_hbm.at[:, k], modes_in.at[k], sems.at[0, k]))
        copies.append(pltpu.make_async_copy(snap_hbm.at[:, k], snap_in.at[k], sems.at[1, k]))
    for c in copies:
        c.start()
    grid = lambda shape: [lax.broadcasted_iota(jnp.int32, shape, d) for d in range(2)]
    row, col = grid((32, 64))
    wanted = (row % 16) // 2 * 8 + row % 2 + jnp.where(row < 16, 0, 6)
    span = (col == wanted).astype(F32).astype(BF16)
    row, col = grid((128, 256))
    last = (col < 128) & (col % 4 < 2) & (row == 126 + col % 4)
    first = (col >= 128) & (col % 4 >= 2) & (row == col % 4 - 2)
    lanes = (last | first).astype(F32).astype(BF16)
    lane = lax.broadcasted_iota(jnp.int32, (16, 128), 1) // 4

    def group_of(group, _):
        units = [snap[8 * group + m] for m in range(8)]
        for pair in range(4):
            both = jnp.concatenate(units[2 * pair : 2 * pair + 2], axis=1)
            picked = jnp.dot(span, both, preferred_element_type=F32).astype(BF16)
            for i in range(2):
                low[8 * group + 2 * pair + i] = picked[:16, 128 * i : 128 * (i + 1)]
                high[8 * group + 2 * pair + i] = picked[16:, 128 * i : 128 * (i + 1)]
        ends = jnp.dot(jnp.concatenate(units, axis=0), lanes, preferred_element_type=F32)
        to_right = jnp.zeros((16, 128), F32)
        to_left = jnp.zeros((16, 128), F32)
        for j in range(32):
            to_right = jnp.where(lane == j, ends[16 * j : 16 * j + 16, :128], to_right)
            to_left = jnp.where(lane == j, ends[16 * j : 16 * j + 16, 128:], to_left)
        right[group] = to_right.astype(BF16)
        left[group] = to_left.astype(BF16)
        return _

    lax.fori_loop(0, 24, group_of, 0, unroll=4)
    for c in copies:
        c.wait()


def side_pack(snap, modes, planes):
    wide, slim = jax.ShapeDtypeStruct((192, 16, 128), BF16), jax.ShapeDtypeStruct((24, 16, 128), BF16)
    return pl.pallas_call(
        side_pack_body,
        out_shape=(
            wide,
            wide,
            slim,
            slim,
            jax.ShapeDtypeStruct((24, 128, 8, 128), BF16),
            jax.ShapeDtypeStruct((24, 64, 8, 128), BF16),
        ),
        in_specs=[resident(), in_hbm(), in_hbm()],
        out_specs=(resident(),) * 6,
        scratch_shapes=[pltpu.SemaphoreType.DMA((2, 24))],
        compiler_params=pltpu.CompilerParams(vmem_limit_bytes=VMEM_LIMIT),
        name="side_pack",
    )(in_vmem(snap), from_hbm(modes), from_hbm(planes))


def same_span(total, half, out):
    lanes = lax.broadcasted_iota(jnp.int32, (64, 128), 1) % 8
    s = lax.broadcasted_iota(jnp.int32, (16, 128), 0)
    at = lax.broadcasted_iota(jnp.int32, (16, 128), 1)
    group = (at // 8 == s).astype(F32)
    for block in range(4):
        kept = total[block, pl.ds(512 * half, 64, stride=8), :]
        for z in range(1, 8):
            kept = jnp.where(lanes == z, total[block, pl.ds(512 * half + z, 64, stride=8), :], kept)
        out[16 * block : 16 * block + 16, 64 * half : 64 * half + 64] = lax.dot_general(
            group, kept, NT, precision=HIGH, preferred_element_type=F32
        )


def add_products(modes, half, planes, data, total, base):
    a = jnp.concatenate([modes[k, 64 * half : 64 * half + 64].reshape(512, 128) for k in planes], axis=1)
    part = lax.dot_general(a, jnp.concatenate(data, axis=1), NT, preferred_element_type=F32)
    rows = slice(512 * half, 512 * half + 512)
    for block in range(4):
        lanes = part[:, 128 * block : 128 * block + 128]
        total[block, rows] = lanes if base is None else base[block, rows] + lanes


def snap_project_body(modes_in, snap_in, out, total):
    for half in range(2):
        for k in range(0, 24, 12):
            planes = range(k, k + 12)
            data = [snap_in[p].reshape(512, 128) for p in planes]
            add_products(modes_in, half, planes, data, total, total if k else None)
        same_span(total, half, out)


def snap_project(modes_in, snap_in):
    return pl.pallas_call(
        snap_project_body,
        out_shape=jax.ShapeDtypeStruct((64, 128), F32),
        in_specs=[resident(), resident()],
        out_specs=resident(),
        scratch_shapes=[pltpu.VMEM((4, 1024, 128), F32)],
        compiler_params=pltpu.CompilerParams(vmem_limit_bytes=VMEM_LIMIT),
        name="snap_project",
    )(in_vmem(modes_in), in_vmem(snap_in))


def feature_body(
    modes_in, snap, z_low, z_high, x_low, x_high, span, stream, masks, total, edges, field
):
    def block(step, _):
        for pair in range(4):
            base = 24 * step + 6 * pair
            units = [[6 * pair + 3 * i + c for c in range(3)] for i in range(2)]
            cells = [[snap[base + 3 * i + c] for c in range(3)] for i in range(2)]
            inside = jnp.concatenate(cells[0] + cells[1], axis=0)
            beside = []
            for u in units[0] + units[1]:
                halo = x_low[3 * step + u // 8] + x_high[3 * step + u // 8]
                beside.append(jnp.concatenate([halo] * 4, axis=0) * masks[u % 8])
            beside = jnp.concatenate(beside, axis=0)
            along = jnp.dot(jnp.concatenate([inside, beside], axis=1), stream[...], preferred_element_type=F32)
            wide = [[v.astype(F32).reshape(8, 8, 128) for v in row] for row in cells]
            velocity = [[v * (1.0 / 12.0) for v in row] for row in wide]
            for c in range(3):
                padded = [
                    jnp.concatenate(
                        [cells[i][c], z_low[base + 3 * i + c], z_high[base + 3 * i + c]], axis=0
                    )
                    for i in range(2)
                ]
                across = jnp.dot(span[...], jnp.concatenate(padded, axis=1), preferred_element_type=F32)
                both = []
                for i in range(2):
                    none = jnp.zeros((2, 8, 128), F32)
                    ext = jnp.concatenate([none, wide[i][c], none], axis=0)
                    near, far = ext[3:11] - ext[1:9], ext[4:12] - ext[0:8]
                    lanes = slice(128 * i, 128 * (i + 1))
                    rows = slice(192 * i + 64 * c, 192 * i + 64 * (c + 1))
                    cube = lambda part: part.reshape(8, 8, 128)
                    laplace = cube(across[0:64, lanes]) + cube(along[rows, 128:256])
                    advect = (
                        velocity[i][0] * cube(along[rows, 0:128])
                        + velocity[i][1] * (8.0 * near - far)
                        + velocity[i][2] * cube(across[64:128, lanes])
                    )
                    value = laplace * (VISCOSITY / 12.0) - advect
                    both.append(value[2:6])
                    edges[base + 3 * i + c, 0:2] = value[0:2]
                    edges[base + 3 * i + c, 2:4] = value[6:8]
                start = pl.multiple_of((8 * step + 2 * pair) * 8, 16)
                field[4 * c : 4 * c + 4, pl.ds(start, 16), :] = jnp.concatenate(both, axis=1).astype(BF16)
        return _

    lax.fori_loop(0, 8, block, 0)
    planes = [8 * c + y for c in range(3) for y in range(2, 6)]
    for half in range(2):
        add_products(modes_in, half, planes, [field[k] for k in range(12)], total, None)


def feature_project(modes_in, snap, z_low, z_high, x_low, x_high):
    consts = [jnp.asarray(v, BF16) for v in (span_operator(), stream_operator(), lane_masks())]
    return pl.pallas_call(
        feature_body,
        out_shape=(
            jax.ShapeDtypeStruct((4, 1024, 128), F32),
            jax.ShapeDtypeStruct((192, 4, 8, 128), F32),
        ),
        in_specs=[resident()] * 9,
        out_specs=(resident(), resident()),
        scratch_shapes=[pltpu.VMEM((12, 512, 128), BF16)],
        compiler_params=pltpu.CompilerParams(vmem_limit_bytes=VMEM_LIMIT),
        name="feature_project",
    )(*map(in_vmem, (modes_in, snap, z_low, z_high, x_low, x_high)), *consts)


def edge_body(modes_in, snap, edges, y_low, y_high, inner, snap_part, mine, other, out, field, total):
    k = VISCOSITY / 12.0
    row = lax.axis_index("gy")
    has_below, has_above = row > 0, row < 3

    def block(step, _):
        base = 12 * step
        values = []
        for i in range(4):
            wall = snap[base + 3 * i + 1].astype(F32) * (1.0 / 12.0)
            wall = wall.reshape(8, 8, 128)
            below_near, below_far = 16.0 * k + 8.0 * wall[0], k + wall[0]
            above_near, above_far = 16.0 * k - 8.0 * wall[7], k - wall[7]
            second, seventh = k + wall[1], k - wall[6]
            row = []
            for c in range(3):
                u = base + 3 * i + c
                below = jnp.where(has_below, y_low[u].astype(F32), 0.0).reshape(2, 8, 128)
                above = jnp.where(has_above, y_high[u].astype(F32), 0.0).reshape(2, 8, 128)
                value = edges[u]
                row.append(
                    jnp.stack(
                        [
                            value[0] + (below_near * below[1] - below_far * below[0]),
                            value[1] - second * below[1],
                            value[2] - seventh * above[0],
                            value[3] + (above_near * above[0] - above_far * above[1]),
                        ]
                    )
                )
            values.append(row)
        for pair in range(2):
            start = pl.multiple_of((4 * step + 2 * pair) * 8, 16)
            for c in range(3):
                both = jnp.concatenate([values[2 * pair][c], values[2 * pair + 1][c]], axis=1)
                field[4 * c : 4 * c + 4, pl.ds(start, 16), :] = both.astype(BF16)
        return _

    lax.fori_loop(0, 16, block, 0, unroll=4)
    planes = [8 * c + y for c in range(3) for y in (0, 1, 6, 7)]
    for half in range(2):
        add_products(modes_in, half, planes, [field[k] for k in range(12)], total, inner)
        same_span(total, half, out)
    first = lax.axis_index("gz_1") == 0
    mine[...] = jnp.where(first, snap_part[...], out[...])
    other[...] = jnp.where(first, out[...], snap_part[...])


def edge_project(modes_in, snap, edges, y_low, y_high, inner, snap_part):
    return pl.pallas_call(
        edge_body,
        out_shape=(jax.ShapeDtypeStruct((64, 128), F32),) * 2,
        in_specs=[resident()] * 7,
        out_specs=(resident(), resident()),
        scratch_shapes=[pltpu.VMEM((64, 128), F32), pltpu.VMEM((12, 512, 128), BF16), pltpu.VMEM((4, 1024, 128), F32)],
        compiler_params=pltpu.CompilerParams(vmem_limit_bytes=VMEM_LIMIT),
        name="edge_project",
    )(*map(in_vmem, (modes_in, snap, edges, y_low, y_high, inner, snap_part)))


def gram_body(mine, other, snap_out, feature_out, gram_snap, gram_feature, gram_quad):
    first = lax.axis_index("gz_1") == 0
    rs = jnp.where(first, mine[...], other[...])
    rf = jnp.where(first, other[...], mine[...])
    snap_out[...] = rs
    feature_out[...] = rf
    dot = functools.partial(lax.dot_general, precision=HIGH, preferred_element_type=F32)
    gram_snap[...] = dot(rs, rs, TN) * (1.0 / 64)
    gram_feature[...] = dot(rf, rs, TN) * (1.0 / 64)
    products = dot(rs, rs, NT) * (1.0 / 128)
    gram_quad[...] = products * products


def grams(mine, other):
    shape = lambda *s: jax.ShapeDtypeStruct(s, F32)
    vmem = pl.BlockSpec(memory_space=pltpu.VMEM)
    return pl.pallas_call(
        gram_body,
        in_specs=[vmem, vmem],
        out_shape=(shape(64, 128), shape(64, 128), shape(128, 128), shape(128, 128), shape(64, 64)),
        compiler_params=pltpu.CompilerParams(vmem_limit_bytes=VMEM_LIMIT),
        name="grams",
    )(in_vmem(mine), in_vmem(other))


def shifted(value, axis, count, by):
    return lax.ppermute(value, axis, [(i, (i + by) % count) for i in range(count)])


def swapped(value, axis, partners):
    return lax.ppermute(value, axis, list(enumerate(partners)))


def other_core(value):
    return lax.ppermute(value, "gz_1", [(0, 1), (1, 0)])


ROUNDS = (
    ("gx", (1, 0, 3, 2)),
    ("gx", (3, 2, 1, 0)),
    ("gy", (1, 0, 3, 2)),
    ("gy", (3, 2, 1, 0)),
    ("gz_0", (1, 0, 3, 2, 5, 4, 7, 6)),
    ("gz_0", (2, 3, 0, 1, 6, 7, 4, 5)),
    ("gz_0", (6, 7, 4, 5, 2, 3, 0, 1)),
)


def shards(snapshots, modes):
    low, high, units = wall_pack(snapshots.reshape(192, 64, 128))
    y_low = shifted(high, "gy", 4, 1)
    y_high = shifted(low, "gy", 4, -1)
    low, high, right, left, modes_in, snap_in = side_pack(
        units, modes.reshape(128, 24, 8, 128), snapshots.reshape(64, 24, 8, 128)
    )
    z_low = shifted(high, GZ, 16, 1)
    z_high = shifted(low, GZ, 16, -1)
    x_low = shifted(right, "gx", 4, 1)
    x_high = shifted(left, "gx", 4, -1)
    snap_part = snap_project(modes_in, snap_in)
    inner, edges = feature_project(modes_in, units, z_low, z_high, x_low, x_high)
    mine, other = edge_project(modes_in, units, edges, y_low, y_high, inner, snap_part)
    total = mine + other_core(other)
    for axis, partners in ROUNDS:
        total = total + swapped(total, axis, partners)
    rs, rf, gram_snap, gram_feature, gram_quad = grams(total, other_core(total))
    return rs.T, rf.T, gram_snap, gram_feature, gram_quad


def solution(mesh):
    finer = Mesh(
        mesh.devices.reshape(mesh.shape["gx"], mesh.shape["gy"], 8, 2), ("gx", "gy", "gz_0", "gz_1")
    )
    placed = (P(None, None, "gy", GZ, "gx"), P(None, None, "gy", GZ, "gx"))

    return jax.shard_map(shards, mesh=finer, in_specs=placed, out_specs=(P(), P(), P(), P(), P()), check_vma=False)
```

```python
import functools

import jax
import jax.numpy as jnp
import numpy as np
from jax import lax
from jax.experimental import pallas as pl
from jax.experimental.pallas import tpu as pltpu
from jax.sharding import Mesh
from jax.sharding import PartitionSpec as P


GZ = ("gz_0", "gz_1")
BF16 = jnp.bfloat16
F32 = jnp.float32
VISCOSITY = 0.1
VMEM_LIMIT = 10 * 2**20
HIGH = lax.Precision.HIGHEST
NT = (((1,), (1,)), ((), ()))
TN = (((0,), (0,)), ((), ()))

GRAD = {-2: 1.0, -1: -8.0, 1: 8.0, 2: -1.0}
CURV = {-2: -1.0, -1: 16.0, 0: -30.0, 1: 16.0, 2: -1.0}


def span_operator():
    op = np.zeros((128, 96), np.float32)

    def column(y, z):
        if z < 0:
            return 64 + y * 2 + z + 2
        if z > 7:
            return 80 + y * 2 + z - 8
        return y * 8 + z

    for y in range(8):
        for z in range(8):
            row = y * 8 + z
            for k, value in CURV.items():
                op[row, column(y, z + k)] += value
                if 0 <= y + k < 8:
                    op[row, column(y + k, z)] += value
            for k, value in GRAD.items():
                op[64 + row, column(y, z + k)] += value
    return op


def stream_operator():
    op = np.zeros((256, 256), np.float32)
    for part, taps in enumerate((GRAD, CURV)):
        for x in range(128):
            for k, value in taps.items():
                at = x + k
                if 0 <= at < 128:
                    op[at, part * 128 + x] += value
                else:
                    halo = at + 2 if at < 0 else at - 128 + 2
                    for j in range(32):
                        op[128 + 4 * j + halo, part * 128 + x] += value
    return op


def lane_masks():
    m, row, lane = np.meshgrid(np.arange(8), np.arange(64), np.arange(128), indexing="ij")
    return (lane // 4 == 4 * m + row // 16).astype(np.float32)


def in_vmem(array):
    return pltpu.with_memory_space_constraint(array, pltpu.VMEM)


def from_hbm(array):
    return pltpu.with_memory_space_constraint(array, pltpu.HBM)


def in_hbm():
    return pl.BlockSpec(memory_space=pltpu.HBM)


def resident():
    return pl.BlockSpec(memory_space=pltpu.VMEM)


def wall_pack_body(snap, low, high, units, sems):
    parts = (pl.ds(0, 16), pl.ds(48, 16), pl.ds(16, 32))
    reads = [pltpu.make_async_copy(snap.at[:, at], units.at[:, at], sems.at[i]) for i, at in enumerate(parts)]
    writes = [
        pltpu.make_async_copy(units.at[:, at], to, sems.at[3 + i]) for i, (at, to) in enumerate(zip(parts, (low, high)))
    ]
    for c in reads:
        c.start()
    for r, w in zip(reads, writes):
        r.wait()
        w.start()
    reads[2].wait()
    for w in writes:
        w.wait()


def wall_pack(snap):
    shape = jax.ShapeDtypeStruct((192, 16, 128), BF16)
    return pl.pallas_call(
        wall_pack_body,
        out_shape=(shape, shape, jax.ShapeDtypeStruct((192, 64, 128), BF16)),
        in_specs=[in_hbm()],
        out_specs=(in_hbm(), in_hbm(), resident()),
        scratch_shapes=[pltpu.SemaphoreType.DMA((5,))],
        compiler_params=pltpu.CompilerParams(vmem_limit_bytes=VMEM_LIMIT),
        name="wall_pack",
    )(from_hbm(snap))


def side_pack_body(snap, modes_hbm, snap_hbm, low, high, right, left, modes_in, snap_in, sems):
    copies = []
    for k in range(24):
        copies.append(pltpu.make_async_copy(modes_hbm.at[:, k], modes_in.at[k], sems.at[0, k]))
        copies.append(pltpu.make_async_copy(snap_hbm.at[:, k], snap_in.at[k], sems.at[1, k]))
    for c in copies:
        c.start()
    grid = lambda shape: [lax.broadcasted_iota(jnp.int32, shape, d) for d in range(2)]
    row, col = grid((32, 64))
    wanted = (row % 16) // 2 * 8 + row % 2 + jnp.where(row < 16, 0, 6)
    span = (col == wanted).astype(F32).astype(BF16)
    row, col = grid((128, 256))
    last = (col < 128) & (col % 4 < 2) & (row == 126 + col % 4)
    first = (col >= 128) & (col % 4 >= 2) & (row == col % 4 - 2)
    lanes = (last | first).astype(F32).astype(BF16)
    lane = lax.broadcasted_iota(jnp.int32, (16, 128), 1) // 4

    def group_of(group, _):
        units = [snap[8 * group + m] for m in range(8)]
        for pair in range(4):
            both = jnp.concatenate(units[2 * pair : 2 * pair + 2], axis=1)
            picked = jnp.dot(span, both, preferred_element_type=F32).astype(BF16)
            for i in range(2):
                low[8 * group + 2 * pair + i] = picked[:16, 128 * i : 128 * (i + 1)]
                high[8 * group + 2 * pair + i] = picked[16:, 128 * i : 128 * (i + 1)]
        ends = jnp.dot(jnp.concatenate(units, axis=0), lanes, preferred_element_type=F32)
        to_right = jnp.zeros((16, 128), F32)
        to_left = jnp.zeros((16, 128), F32)
        for j in range(32):
            to_right = jnp.where(lane == j, ends[16 * j : 16 * j + 16, :128], to_right)
            to_left = jnp.where(lane == j, ends[16 * j : 16 * j + 16, 128:], to_left)
        right[group] = to_right.astype(BF16)
        left[group] = to_left.astype(BF16)
        return _

    lax.fori_loop(0, 24, group_of, 0, unroll=4)
    for c in copies:
        c.wait()


def side_pack(snap, modes, planes):
    wide, slim = jax.ShapeDtypeStruct((192, 16, 128), BF16), jax.ShapeDtypeStruct((24, 16, 128), BF16)
    return pl.pallas_call(
        side_pack_body,
        out_shape=(
            wide,
            wide,
            slim,
            slim,
            jax.ShapeDtypeStruct((24, 128, 8, 128), BF16),
            jax.ShapeDtypeStruct((24, 64, 8, 128), BF16),
        ),
        in_specs=[resident(), in_hbm(), in_hbm()],
        out_specs=(resident(),) * 6,
        scratch_shapes=[pltpu.SemaphoreType.DMA((2, 24))],
        compiler_params=pltpu.CompilerParams(vmem_limit_bytes=VMEM_LIMIT),
        name="side_pack",
    )(in_vmem(snap), from_hbm(modes), from_hbm(planes))


def same_span(total, half, out):
    lanes = lax.broadcasted_iota(jnp.int32, (64, 128), 1) % 8
    s = lax.broadcasted_iota(jnp.int32, (16, 128), 0)
    at = lax.broadcasted_iota(jnp.int32, (16, 128), 1)
    group = (at // 8 == s).astype(F32)
    for block in range(4):
        kept = total[block, pl.ds(512 * half, 64, stride=8), :]
        for z in range(1, 8):
            kept = jnp.where(lanes == z, total[block, pl.ds(512 * half + z, 64, stride=8), :], kept)
        out[16 * block : 16 * block + 16, 64 * half : 64 * half + 64] = lax.dot_general(
            group, kept, NT, precision=HIGH, preferred_element_type=F32
        )


def add_products(modes, half, planes, data, total, base):
    a = jnp.concatenate([modes[k, 64 * half : 64 * half + 64].reshape(512, 128) for k in planes], axis=1)
    part = lax.dot_general(a, jnp.concatenate(data, axis=1), NT, preferred_element_type=F32)
    rows = slice(512 * half, 512 * half + 512)
    for block in range(4):
        lanes = part[:, 128 * block : 128 * block + 128]
        total[block, rows] = lanes if base is None else base[block, rows] + lanes


def snap_project_body(modes_in, snap_in, out, total):
    for half in range(2):
        for k in range(0, 24, 12):
            planes = range(k, k + 12)
            data = [snap_in[p].reshape(512, 128) for p in planes]
            add_products(modes_in, half, planes, data, total, total if k else None)
        same_span(total, half, out)


def snap_project(modes_in, snap_in):
    return pl.pallas_call(
        snap_project_body,
        out_shape=jax.ShapeDtypeStruct((64, 128), F32),
        in_specs=[resident(), resident()],
        out_specs=resident(),
        scratch_shapes=[pltpu.VMEM((4, 1024, 128), F32)],
        compiler_params=pltpu.CompilerParams(vmem_limit_bytes=VMEM_LIMIT),
        name="snap_project",
    )(in_vmem(modes_in), in_vmem(snap_in))


def feature_body(
    modes_in, snap, z_low, z_high, x_low, x_high, span, stream, masks, total, edges, field
):
    def block(step, _):
        for pair in range(4):
            base = 24 * step + 6 * pair
            units = [[6 * pair + 3 * i + c for c in range(3)] for i in range(2)]
            cells = [[snap[base + 3 * i + c] for c in range(3)] for i in range(2)]
            inside = jnp.concatenate(cells[0] + cells[1], axis=0)
            beside = []
            for u in units[0] + units[1]:
                halo = x_low[3 * step + u // 8] + x_high[3 * step + u // 8]
                beside.append(jnp.concatenate([halo] * 4, axis=0) * masks[u % 8])
            beside = jnp.concatenate(beside, axis=0)
            along = jnp.dot(jnp.concatenate([inside, beside], axis=1), stream[...], preferred_element_type=F32)
            wide = [[v.astype(F32).reshape(8, 8, 128) for v in row] for row in cells]
            velocity = [[v * (1.0 / 12.0) for v in row] for row in wide]
            for c in range(3):
                padded = [
                    jnp.concatenate(
                        [cells[i][c], z_low[base + 3 * i + c], z_high[base + 3 * i + c]], axis=0
                    )
                    for i in range(2)
                ]
                across = jnp.dot(span[...], jnp.concatenate(padded, axis=1), preferred_element_type=F32)
                both = []
                for i in range(2):
                    none = jnp.zeros((2, 8, 128), F32)
                    ext = jnp.concatenate([none, wide[i][c], none], axis=0)
                    near, far = ext[3:11] - ext[1:9], ext[4:12] - ext[0:8]
                    lanes = slice(128 * i, 128 * (i + 1))
                    rows = slice(192 * i + 64 * c, 192 * i + 64 * (c + 1))
                    cube = lambda part: part.reshape(8, 8, 128)
                    laplace = cube(across[0:64, lanes]) + cube(along[rows, 128:256])
                    advect = (
                        velocity[i][0] * cube(along[rows, 0:128])
                        + velocity[i][1] * (8.0 * near - far)
                        + velocity[i][2] * cube(across[64:128, lanes])
                    )
                    value = laplace * (VISCOSITY / 12.0) - advect
                    both.append(value[2:6])
                    edges[base + 3 * i + c, 0:2] = value[0:2]
                    edges[base + 3 * i + c, 2:4] = value[6:8]
                start = pl.multiple_of((8 * step + 2 * pair) * 8, 16)
                field[4 * c : 4 * c + 4, pl.ds(start, 16), :] = jnp.concatenate(both, axis=1).astype(BF16)
        return _

    lax.fori_loop(0, 8, block, 0)
    planes = [8 * c + y for c in range(3) for y in range(2, 6)]
    for half in range(2):
        add_products(modes_in, half, planes, [field[k] for k in range(12)], total, None)


def feature_project(modes_in, snap, z_low, z_high, x_low, x_high):
    consts = [jnp.asarray(v, BF16) for v in (span_operator(), stream_operator(), lane_masks())]
    return pl.pallas_call(
        feature_body,
        out_shape=(
            jax.ShapeDtypeStruct((4, 1024, 128), F32),
            jax.ShapeDtypeStruct((192, 4, 8, 128), F32),
        ),
        in_specs=[resident()] * 9,
        out_specs=(resident(), resident()),
        scratch_shapes=[pltpu.VMEM((12, 512, 128), BF16)],
        compiler_params=pltpu.CompilerParams(vmem_limit_bytes=VMEM_LIMIT),
        name="feature_project",
    )(*map(in_vmem, (modes_in, snap, z_low, z_high, x_low, x_high)), *consts)


def edge_body(modes_in, snap, edges, y_low, y_high, inner, snap_part, mine, other, out, field, total):
    k = VISCOSITY / 12.0
    row = lax.axis_index("gy")
    has_below, has_above = row > 0, row < 3

    def block(step, _):
        base = 12 * step
        values = []
        for i in range(4):
            wall = snap[base + 3 * i + 1].astype(F32) * (1.0 / 12.0)
            wall = wall.reshape(8, 8, 128)
            below_near, below_far = 16.0 * k + 8.0 * wall[0], k + wall[0]
            above_near, above_far = 16.0 * k - 8.0 * wall[7], k - wall[7]
            second, seventh = k + wall[1], k - wall[6]
            row = []
            for c in range(3):
                u = base + 3 * i + c
                below = jnp.where(has_below, y_low[u].astype(F32), 0.0).reshape(2, 8, 128)
                above = jnp.where(has_above, y_high[u].astype(F32), 0.0).reshape(2, 8, 128)
                value = edges[u]
                row.append(
                    jnp.stack(
                        [
                            value[0] + (below_near * below[1] - below_far * below[0]),
                            value[1] - second * below[1],
                            value[2] - seventh * above[0],
                            value[3] + (above_near * above[0] - above_far * above[1]),
                        ]
                    )
                )
            values.append(row)
        for pair in range(2):
            start = pl.multiple_of((4 * step + 2 * pair) * 8, 16)
            for c in range(3):
                both = jnp.concatenate([values[2 * pair][c], values[2 * pair + 1][c]], axis=1)
                field[4 * c : 4 * c + 4, pl.ds(start, 16), :] = both.astype(BF16)
        return _

    lax.fori_loop(0, 16, block, 0, unroll=4)
    planes = [8 * c + y for c in range(3) for y in (0, 1, 6, 7)]
    for half in range(2):
        add_products(modes_in, half, planes, [field[k] for k in range(12)], total, inner)
        same_span(total, half, out)
    first = snap_half_here()
    mine[...] = jnp.where(first, snap_part[...], out[...])
    other[...] = jnp.where(first, out[...], snap_part[...])


def edge_project(modes_in, snap, edges, y_low, y_high, inner, snap_part):
    return pl.pallas_call(
        edge_body,
        out_shape=(jax.ShapeDtypeStruct((64, 128), F32),) * 2,
        in_specs=[resident()] * 7,
        out_specs=(resident(), resident()),
        scratch_shapes=[pltpu.VMEM((64, 128), F32), pltpu.VMEM((12, 512, 128), BF16), pltpu.VMEM((4, 1024, 128), F32)],
        compiler_params=pltpu.CompilerParams(vmem_limit_bytes=VMEM_LIMIT),
        name="edge_project",
    )(*map(in_vmem, (modes_in, snap, edges, y_low, y_high, inner, snap_part)))


def gram_body(mine, other, snap_out, feature_out, gram_snap, gram_feature, gram_quad):
    first = snap_half_here()
    rs = jnp.where(first, mine[...], other[...])
    rf = jnp.where(first, other[...], mine[...])
    snap_out[...] = rs
    feature_out[...] = rf
    dot = functools.partial(lax.dot_general, precision=HIGH, preferred_element_type=F32)
    gram_snap[...] = dot(rs, rs, TN) * (1.0 / 64)
    gram_feature[...] = dot(rf, rs, TN) * (1.0 / 64)
    products = dot(rs, rs, NT) * (1.0 / 128)
    gram_quad[...] = products * products


def grams(mine, other):
    shape = lambda *s: jax.ShapeDtypeStruct(s, F32)
    vmem = pl.BlockSpec(memory_space=pltpu.VMEM)
    return pl.pallas_call(
        gram_body,
        in_specs=[vmem, vmem],
        out_shape=(shape(64, 128), shape(64, 128), shape(128, 128), shape(128, 128), shape(64, 64)),
        compiler_params=pltpu.CompilerParams(vmem_limit_bytes=VMEM_LIMIT),
        name="grams",
    )(in_vmem(mine), in_vmem(other))


def shifted(value, axis, count, by):
    return lax.ppermute(value, axis, [(i, (i + by) % count) for i in range(count)])


def snap_half_here():
    x, y, z = (lax.axis_index(a) for a in ("gx", "gy", "gz_0"))
    return (lax.axis_index("gz_1") + x + y + z + z // 2) % 2 == 0


def swapped(value, axis, partners):
    pairs = [(2 * i + core, 2 * p + 1 - core) for i, p in enumerate(partners) for core in range(2)]
    return lax.ppermute(value, (axis, "gz_1"), pairs)


def other_core(value):
    return lax.ppermute(value, "gz_1", [(0, 1), (1, 0)])


ROUNDS = (
    ("gx", (1, 0, 3, 2)),
    ("gx", (3, 2, 1, 0)),
    ("gy", (1, 0, 3, 2)),
    ("gy", (3, 2, 1, 0)),
    ("gz_0", (1, 0, 3, 2, 5, 4, 7, 6)),
    ("gz_0", (2, 3, 0, 1, 6, 7, 4, 5)),
    ("gz_0", (6, 7, 4, 5, 2, 3, 0, 1)),
)


def shards(snapshots, modes):
    low, high, units = wall_pack(snapshots.reshape(192, 64, 128))
    y_low = shifted(high, "gy", 4, 1)
    y_high = shifted(low, "gy", 4, -1)
    low, high, right, left, modes_in, snap_in = side_pack(
        units, modes.reshape(128, 24, 8, 128), snapshots.reshape(64, 24, 8, 128)
    )
    z_low = shifted(high, GZ, 16, 1)
    z_high = shifted(low, GZ, 16, -1)
    x_low = shifted(right, "gx", 4, 1)
    x_high = shifted(left, "gx", 4, -1)
    snap_part = snap_project(modes_in, snap_in)
    inner, edges = feature_project(modes_in, units, z_low, z_high, x_low, x_high)
    mine, other = edge_project(modes_in, units, edges, y_low, y_high, inner, snap_part)
    total = mine + other_core(other)
    for axis, partners in ROUNDS:
        total = total + swapped(total, axis, partners)
    rs, rf, gram_snap, gram_feature, gram_quad = grams(total, other_core(total))
    return rs.T, rf.T, gram_snap, gram_feature, gram_quad


def solution(mesh):
    finer = Mesh(
        mesh.devices.reshape(mesh.shape["gx"], mesh.shape["gy"], 8, 2), ("gx", "gy", "gz_0", "gz_1")
    )
    placed = (P(None, None, "gy", GZ, "gx"), P(None, None, "gy", GZ, "gx"))

    return jax.shard_map(shards, mesh=finer, in_specs=placed, out_specs=(P(), P(), P(), P(), P()), check_vma=False)
```

```python
import functools

import jax
import jax.numpy as jnp
import numpy as np
from jax import lax
from jax.experimental import pallas as pl
from jax.experimental.pallas import tpu as pltpu
from jax.sharding import Mesh
from jax.sharding import PartitionSpec as P


GZ = ("gz_0", "gz_1")
BF16 = jnp.bfloat16
F32 = jnp.float32
VISCOSITY = 0.1
VMEM_LIMIT = 10 * 2**20
HIGH = lax.Precision.HIGHEST
NT = (((1,), (1,)), ((), ()))
TN = (((0,), (0,)), ((), ()))

GRAD = {-2: 1.0, -1: -8.0, 1: 8.0, 2: -1.0}
CURV = {-2: -1.0, -1: 16.0, 0: -30.0, 1: 16.0, 2: -1.0}


def span_operator():
    op = np.zeros((128, 96), np.float32)

    def column(y, z):
        if z < 0:
            return 64 + y * 2 + z + 2
        if z > 7:
            return 80 + y * 2 + z - 8
        return y * 8 + z

    for y in range(8):
        for z in range(8):
            row = y * 8 + z
            for k, value in CURV.items():
                op[row, column(y, z + k)] += value
                if 0 <= y + k < 8:
                    op[row, column(y + k, z)] += value
            for k, value in GRAD.items():
                op[64 + row, column(y, z + k)] += value
    return op


def stream_operator():
    op = np.zeros((256, 256), np.float32)
    for part, taps in enumerate((GRAD, CURV)):
        for x in range(128):
            for k, value in taps.items():
                at = x + k
                if 0 <= at < 128:
                    op[at, part * 128 + x] += value
                else:
                    halo = at + 2 if at < 0 else at - 128 + 2
                    for j in range(32):
                        op[128 + 4 * j + halo, part * 128 + x] += value
    return op


def lane_masks():
    m, row, lane = np.meshgrid(np.arange(8), np.arange(64), np.arange(128), indexing="ij")
    return (lane // 4 == 4 * m + row // 16).astype(np.float32)


def in_vmem(array):
    return pltpu.with_memory_space_constraint(array, pltpu.VMEM)


def from_hbm(array):
    return pltpu.with_memory_space_constraint(array, pltpu.HBM)


def in_hbm():
    return pl.BlockSpec(memory_space=pltpu.HBM)


def resident():
    return pl.BlockSpec(memory_space=pltpu.VMEM)


def wall_pack_body(snap, low, high, units, sems):
    parts = (pl.ds(0, 16), pl.ds(48, 16), pl.ds(16, 32))
    reads = [pltpu.make_async_copy(snap.at[:, at], units.at[:, at], sems.at[i]) for i, at in enumerate(parts)]
    writes = [
        pltpu.make_async_copy(units.at[:, at], to, sems.at[3 + i]) for i, (at, to) in enumerate(zip(parts, (low, high)))
    ]
    for c in reads:
        c.start()
    for r, w in zip(reads, writes):
        r.wait()
        w.start()
    reads[2].wait()
    for w in writes:
        w.wait()


def wall_pack(snap):
    shape = jax.ShapeDtypeStruct((192, 16, 128), BF16)
    return pl.pallas_call(
        wall_pack_body,
        out_shape=(shape, shape, jax.ShapeDtypeStruct((192, 64, 128), BF16)),
        in_specs=[in_hbm()],
        out_specs=(in_hbm(), in_hbm(), resident()),
        scratch_shapes=[pltpu.SemaphoreType.DMA((5,))],
        compiler_params=pltpu.CompilerParams(vmem_limit_bytes=VMEM_LIMIT),
        name="wall_pack",
    )(from_hbm(snap))


def plane_copies(array, planes, sems):
    return [pltpu.make_async_copy(array.at[:, k], planes.at[k], sems.at[k]) for k in range(24)]


def span_pack_body(snap, snap_hbm, low, high, snap_in, sems):
    copies = plane_copies(snap_hbm, snap_in, sems)
    for c in copies:
        c.start()
    row, col = (lax.broadcasted_iota(jnp.int32, (32, 64), d) for d in range(2))
    wanted = (row % 16) // 2 * 8 + row % 2 + jnp.where(row < 16, 0, 6)
    span = (col == wanted).astype(F32).astype(BF16)

    def group_of(group, _):
        for pair in range(4):
            unit = 8 * group + 2 * pair
            both = jnp.concatenate([snap[unit], snap[unit + 1]], axis=1)
            picked = jnp.dot(span, both, preferred_element_type=F32).astype(BF16)
            for i in range(2):
                low[unit + i] = picked[:16, 128 * i : 128 * (i + 1)]
                high[unit + i] = picked[16:, 128 * i : 128 * (i + 1)]
        return _

    lax.fori_loop(0, 24, group_of, 0, unroll=4)
    for c in copies:
        c.wait()


def stream_pack_body(snap, modes_hbm, right, left, modes_in, sems):
    copies = plane_copies(modes_hbm, modes_in, sems)
    for c in copies:
        c.start()
    row, col = (lax.broadcasted_iota(jnp.int32, (128, 256), d) for d in range(2))
    last = (col < 128) & (col % 4 < 2) & (row == 126 + col % 4)
    first = (col >= 128) & (col % 4 >= 2) & (row == col % 4 - 2)
    lanes = (last | first).astype(F32).astype(BF16)
    lane = lax.broadcasted_iota(jnp.int32, (16, 128), 1) // 4

    def group_of(group, _):
        units = [snap[8 * group + m] for m in range(8)]
        ends = jnp.dot(jnp.concatenate(units, axis=0), lanes, preferred_element_type=F32)
        to_right = jnp.zeros((16, 128), F32)
        to_left = jnp.zeros((16, 128), F32)
        for j in range(32):
            to_right = jnp.where(lane == j, ends[16 * j : 16 * j + 16, :128], to_right)
            to_left = jnp.where(lane == j, ends[16 * j : 16 * j + 16, 128:], to_left)
        right[group] = to_right.astype(BF16)
        left[group] = to_left.astype(BF16)
        return _

    lax.fori_loop(0, 24, group_of, 0, unroll=4)
    for c in copies:
        c.wait()


def packed(body, rows, snap, array):
    halo = jax.ShapeDtypeStruct((rows, 16, 128), BF16)
    return pl.pallas_call(
        body,
        out_shape=(halo, halo, jax.ShapeDtypeStruct((24, array.shape[0], 8, 128), BF16)),
        in_specs=[resident(), in_hbm()],
        out_specs=(resident(),) * 3,
        scratch_shapes=[pltpu.SemaphoreType.DMA((24,))],
        compiler_params=pltpu.CompilerParams(vmem_limit_bytes=VMEM_LIMIT),
    )(in_vmem(snap), from_hbm(array))


def same_span(total, half, out):
    lanes = lax.broadcasted_iota(jnp.int32, (64, 128), 1) % 8
    s = lax.broadcasted_iota(jnp.int32, (16, 128), 0)
    at = lax.broadcasted_iota(jnp.int32, (16, 128), 1)
    group = (at // 8 == s).astype(F32)
    for block in range(4):
        kept = total[block, pl.ds(512 * half, 64, stride=8), :]
        for z in range(1, 8):
            kept = jnp.where(lanes == z, total[block, pl.ds(512 * half + z, 64, stride=8), :], kept)
        out[16 * block : 16 * block + 16, 64 * half : 64 * half + 64] = lax.dot_general(
            group, kept, NT, precision=HIGH, preferred_element_type=F32
        )


def add_products(modes, half, planes, data, total, base):
    a = jnp.concatenate([modes[k, 64 * half : 64 * half + 64].reshape(512, 128) for k in planes], axis=1)
    part = lax.dot_general(a, jnp.concatenate(data, axis=1), NT, preferred_element_type=F32)
    rows = slice(512 * half, 512 * half + 512)
    for block in range(4):
        lanes = part[:, 128 * block : 128 * block + 128]
        total[block, rows] = lanes if base is None else base[block, rows] + lanes


def snap_project_body(modes_in, snap_in, out, total):
    for half in range(2):
        for k in range(0, 24, 12):
            planes = range(k, k + 12)
            data = [snap_in[p].reshape(512, 128) for p in planes]
            add_products(modes_in, half, planes, data, total, total if k else None)
        same_span(total, half, out)


def snap_project(modes_in, snap_in):
    return pl.pallas_call(
        snap_project_body,
        out_shape=jax.ShapeDtypeStruct((64, 128), F32),
        in_specs=[resident(), resident()],
        out_specs=resident(),
        scratch_shapes=[pltpu.VMEM((4, 1024, 128), F32)],
        compiler_params=pltpu.CompilerParams(vmem_limit_bytes=VMEM_LIMIT),
        name="snap_project",
    )(in_vmem(modes_in), in_vmem(snap_in))


def feature_body(
    modes_in, snap, z_low, z_high, x_low, x_high, span, stream, masks, total, edges, field
):
    def block(step, _):
        for pair in range(4):
            base = 24 * step + 6 * pair
            units = [[6 * pair + 3 * i + c for c in range(3)] for i in range(2)]
            cells = [[snap[base + 3 * i + c] for c in range(3)] for i in range(2)]
            inside = jnp.concatenate(cells[0] + cells[1], axis=0)
            beside = []
            for u in units[0] + units[1]:
                halo = x_low[3 * step + u // 8] + x_high[3 * step + u // 8]
                beside.append(jnp.concatenate([halo] * 4, axis=0) * masks[u % 8])
            beside = jnp.concatenate(beside, axis=0)
            along = jnp.dot(jnp.concatenate([inside, beside], axis=1), stream[...], preferred_element_type=F32)
            wide = [[v.astype(F32).reshape(8, 8, 128) for v in row] for row in cells]
            velocity = [[v * (1.0 / 12.0) for v in row] for row in wide]
            for c in range(3):
                padded = [
                    jnp.concatenate(
                        [cells[i][c], z_low[base + 3 * i + c], z_high[base + 3 * i + c]], axis=0
                    )
                    for i in range(2)
                ]
                across = jnp.dot(span[...], jnp.concatenate(padded, axis=1), preferred_element_type=F32)
                both = []
                for i in range(2):
                    none = jnp.zeros((2, 8, 128), F32)
                    ext = jnp.concatenate([none, wide[i][c], none], axis=0)
                    near, far = ext[3:11] - ext[1:9], ext[4:12] - ext[0:8]
                    lanes = slice(128 * i, 128 * (i + 1))
                    rows = slice(192 * i + 64 * c, 192 * i + 64 * (c + 1))
                    cube = lambda part: part.reshape(8, 8, 128)
                    laplace = cube(across[0:64, lanes]) + cube(along[rows, 128:256])
                    advect = (
                        velocity[i][0] * cube(along[rows, 0:128])
                        + velocity[i][1] * (8.0 * near - far)
                        + velocity[i][2] * cube(across[64:128, lanes])
                    )
                    value = laplace * (VISCOSITY / 12.0) - advect
                    both.append(value[2:6])
                    edges[base + 3 * i + c, 0:2] = value[0:2]
                    edges[base + 3 * i + c, 2:4] = value[6:8]
                start = pl.multiple_of((8 * step + 2 * pair) * 8, 16)
                field[4 * c : 4 * c + 4, pl.ds(start, 16), :] = jnp.concatenate(both, axis=1).astype(BF16)
        return _

    lax.fori_loop(0, 8, block, 0)
    planes = [8 * c + y for c in range(3) for y in range(2, 6)]
    for half in range(2):
        add_products(modes_in, half, planes, [field[k] for k in range(12)], total, None)


def feature_project(modes_in, snap, z_low, z_high, x_low, x_high):
    consts = [jnp.asarray(v, BF16) for v in (span_operator(), stream_operator(), lane_masks())]
    return pl.pallas_call(
        feature_body,
        out_shape=(
            jax.ShapeDtypeStruct((4, 1024, 128), F32),
            jax.ShapeDtypeStruct((192, 4, 8, 128), F32),
        ),
        in_specs=[resident()] * 9,
        out_specs=(resident(), resident()),
        scratch_shapes=[pltpu.VMEM((12, 512, 128), BF16)],
        compiler_params=pltpu.CompilerParams(vmem_limit_bytes=VMEM_LIMIT),
        name="feature_project",
    )(*map(in_vmem, (modes_in, snap, z_low, z_high, x_low, x_high)), *consts)


def edge_body(modes_in, snap, edges, y_low, y_high, inner, snap_part, mine, other, out, field, total):
    k = VISCOSITY / 12.0
    row = lax.axis_index("gy")
    has_below, has_above = row > 0, row < 3

    def block(step, _):
        base = 12 * step
        values = []
        for i in range(4):
            wall = snap[base + 3 * i + 1].astype(F32) * (1.0 / 12.0)
            wall = wall.reshape(8, 8, 128)
            below_near, below_far = 16.0 * k + 8.0 * wall[0], k + wall[0]
            above_near, above_far = 16.0 * k - 8.0 * wall[7], k - wall[7]
            second, seventh = k + wall[1], k - wall[6]
            row = []
            for c in range(3):
                u = base + 3 * i + c
                below = jnp.where(has_below, y_low[u].astype(F32), 0.0).reshape(2, 8, 128)
                above = jnp.where(has_above, y_high[u].astype(F32), 0.0).reshape(2, 8, 128)
                value = edges[u]
                row.append(
                    jnp.stack(
                        [
                            value[0] + (below_near * below[1] - below_far * below[0]),
                            value[1] - second * below[1],
                            value[2] - seventh * above[0],
                            value[3] + (above_near * above[0] - above_far * above[1]),
                        ]
                    )
                )
            values.append(row)
        for pair in range(2):
            start = pl.multiple_of((4 * step + 2 * pair) * 8, 16)
            for c in range(3):
                both = jnp.concatenate([values[2 * pair][c], values[2 * pair + 1][c]], axis=1)
                field[4 * c : 4 * c + 4, pl.ds(start, 16), :] = both.astype(BF16)
        return _

    lax.fori_loop(0, 16, block, 0, unroll=4)
    planes = [8 * c + y for c in range(3) for y in (0, 1, 6, 7)]
    for half in range(2):
        add_products(modes_in, half, planes, [field[k] for k in range(12)], total, inner)
        same_span(total, half, out)
    first = snap_half_here()
    mine[...] = jnp.where(first, snap_part[...], out[...])
    other[...] = jnp.where(first, out[...], snap_part[...])


def edge_project(modes_in, snap, edges, y_low, y_high, inner, snap_part):
    return pl.pallas_call(
        edge_body,
        out_shape=(jax.ShapeDtypeStruct((64, 128), F32),) * 2,
        in_specs=[resident()] * 7,
        out_specs=(resident(), resident()),
        scratch_shapes=[pltpu.VMEM((64, 128), F32), pltpu.VMEM((12, 512, 128), BF16), pltpu.VMEM((4, 1024, 128), F32)],
        compiler_params=pltpu.CompilerParams(vmem_limit_bytes=VMEM_LIMIT),
        name="edge_project",
    )(*map(in_vmem, (modes_in, snap, edges, y_low, y_high, inner, snap_part)))


def gram_body(mine, other, snap_out, feature_out, gram_snap, gram_feature, gram_quad):
    first = snap_half_here()
    rs = jnp.where(first, mine[...], other[...])
    rf = jnp.where(first, other[...], mine[...])
    snap_out[...] = rs
    feature_out[...] = rf
    dot = functools.partial(lax.dot_general, precision=HIGH, preferred_element_type=F32)
    gram_snap[...] = dot(rs, rs, TN) * (1.0 / 64)
    gram_feature[...] = dot(rf, rs, TN) * (1.0 / 64)
    products = dot(rs, rs, NT) * (1.0 / 128)
    gram_quad[...] = products * products


def grams(mine, other):
    shape = lambda *s: jax.ShapeDtypeStruct(s, F32)
    vmem = pl.BlockSpec(memory_space=pltpu.VMEM)
    return pl.pallas_call(
        gram_body,
        in_specs=[vmem, vmem],
        out_shape=(shape(64, 128), shape(64, 128), shape(128, 128), shape(128, 128), shape(64, 64)),
        compiler_params=pltpu.CompilerParams(vmem_limit_bytes=VMEM_LIMIT),
        name="grams",
    )(in_vmem(mine), in_vmem(other))


def shifted(value, axis, count, by):
    return lax.ppermute(value, axis, [(i, (i + by) % count) for i in range(count)])


def snap_half_here():
    x, y, z = (lax.axis_index(a) for a in ("gx", "gy", "gz_0"))
    return (lax.axis_index("gz_1") + x + y + z + z // 2) % 2 == 0


def swapped(value, axis, partners):
    pairs = [(2 * i + core, 2 * p + 1 - core) for i, p in enumerate(partners) for core in range(2)]
    return lax.ppermute(value, (axis, "gz_1"), pairs)


def other_core(value):
    return lax.ppermute(value, "gz_1", [(0, 1), (1, 0)])


ROUNDS = (
    ("gx", (1, 0, 3, 2)),
    ("gx", (3, 2, 1, 0)),
    ("gy", (1, 0, 3, 2)),
    ("gy", (3, 2, 1, 0)),
    ("gz_0", (1, 0, 3, 2, 5, 4, 7, 6)),
    ("gz_0", (2, 3, 0, 1, 6, 7, 4, 5)),
    ("gz_0", (6, 7, 4, 5, 2, 3, 0, 1)),
)


def shards(snapshots, modes):
    low, high, units = wall_pack(snapshots.reshape(192, 64, 128))
    y_low = shifted(high, "gy", 4, 1)
    y_high = shifted(low, "gy", 4, -1)
    low, high, snap_in = packed(span_pack_body, 192, units, snapshots.reshape(64, 24, 8, 128))
    z_low = shifted(high, GZ, 16, 1)
    z_high = shifted(low, GZ, 16, -1)
    right, left, modes_in = packed(stream_pack_body, 24, units, modes.reshape(128, 24, 8, 128))
    x_low = shifted(right, "gx", 4, 1)
    x_high = shifted(left, "gx", 4, -1)
    snap_part = snap_project(modes_in, snap_in)
    inner, edges = feature_project(modes_in, units, z_low, z_high, x_low, x_high)
    mine, other = edge_project(modes_in, units, edges, y_low, y_high, inner, snap_part)
    total = mine + other_core(other)
    for axis, partners in ROUNDS:
        total = total + swapped(total, axis, partners)
    rs, rf, gram_snap, gram_feature, gram_quad = grams(total, other_core(total))
    return rs.T, rf.T, gram_snap, gram_feature, gram_quad


def solution(mesh):
    finer = Mesh(
        mesh.devices.reshape(mesh.shape["gx"], mesh.shape["gy"], 8, 2), ("gx", "gy", "gz_0", "gz_1")
    )
    placed = (P(None, None, "gy", GZ, "gx"), P(None, None, "gy", GZ, "gx"))

    return jax.shard_map(shards, mesh=finer, in_specs=placed, out_specs=(P(), P(), P(), P(), P()), check_vma=False)
```
